512 devices in a mesh: lon: 32 (over y, x_hi, core), lat: 16 (over x_lo, z).
Axes of the slice: x: 4 (x_hi: 2, x_lo: 2; x = x_hi * 2 + x_lo), y: 8, z: 8, core: 2. Of those that a mesh axis runs over, the one named last changes fastest.
Arguments:
- latent: bfloat16 [4, 256, 512, 320], P(None, 'lat', 'lon'), may hold values from -28 to 28, as said below
- norm1_gain: float32 [320], replicated, may hold values from 0.1 to 1.9
- norm1_shift: float32 [320], replicated, may hold values from -3 to 3
- conv1_weight: bfloat16 [3, 3, 320, 320], replicated, may hold values from -0.109375 to 0.109375
- conv1_bias: float32 [320], replicated, may hold values from -3 to 3
- emb_shift: float32 [4, 320], replicated, may hold values from -4 to 4
- norm2_gain: float32 [320], replicated, may hold values from 0.1 to 1.9
- norm2_shift: float32 [320], replicated, may hold values from -3 to 3
- conv2_weight: bfloat16 [3, 3, 320, 320], replicated, may hold values from -0.109375 to 0.109375
- conv2_bias: float32 [320], replicated, may hold values from -3 to 3
Outputs:
- block_out: bfloat16 [4, 256, 512, 320], P(None, 'lat', 'lon')
The draws below stay inside these ranges and needn't reach their ends.
Inputs may be any that keep to these rules, and one draw needn't show every extreme that they name: `latent`: Real-valued activations.
All inputs are finite; a program needn't handle non-finite values.
Results may differ from the reference program's by a relative error of at most 0.007.
Values may be sent and summed in bfloat16 or wider, within the bound.
A program may use at most 64 MiB of HBM per device.

```python
import jax
import jax.numpy as jnp
from jax import lax

C = 320
GROUPS = 32
FRAMES = 4
LAT_ROWS = 256
LON_COLS = 512


def draw_latent(key, part):
    noise_key = jax.random.fold_in(key, 11)
    lat_key = jax.random.fold_in(key, 12)
    lon_key = jax.random.fold_in(key, 13)
    offset_key = jax.random.fold_in(key, 14)
    lat_frac = jnp.arange(LAT_ROWS, dtype=jnp.float32) / LAT_ROWS
    lon_frac = jnp.arange(LON_COLS, dtype=jnp.float32) / LON_COLS
    rough_lat = jax.random.uniform(lat_key, (LAT_ROWS,), jnp.float32, 0.8, 1.25)
    rough_lon = jax.random.uniform(lon_key, (LON_COLS,), jnp.float32, 0.8, 1.25)
    scales = 0.3 * (3.0 ** lat_frac * rough_lat)[:, None] * (3.0 ** lon_frac * rough_lon)[None, :]
    offset = jnp.clip(0.5 * jax.random.normal(offset_key, (C,), jnp.float32), -1.5, 1.5)
    noise_draw = jnp.clip(jax.random.normal(noise_key, (FRAMES, LAT_ROWS, LON_COLS, C), jnp.float32), -5.0, 5.0)
    return (scales[None, :, :, None] * (noise_draw + offset)).astype(jnp.bfloat16)


def noise(key, extent, spread, limit, held_as=jnp.bfloat16):
    entries = spread * jax.random.normal(key, extent, jnp.float32)
    return jnp.clip(entries, min=-limit, max=limit).astype(held_as)


def setup_inputs(seed: int = 0) -> dict:
    key_list = jax.random.split(jax.random.key(seed), 11)
    latent = draw_latent(jax.random.fold_in(key_list[10], 71), 0)
    norm1_gain = jnp.clip(1.0 + 0.18 * jax.random.normal(key_list[1], (C,), jnp.float32), 0.1, 1.9)
    norm1_shift = noise(key_list[2], (C,), 0.5, 3.0, jnp.float32)
    conv1_weight = noise(key_list[3], (3, 3, C, C), (9 * C) ** -0.5, 0.109375)
    conv1_bias = noise(key_list[4], (C,), 0.5, 3.0, jnp.float32)
    emb_shift = noise(key_list[5], (FRAMES, C), 1.0, 4.0, jnp.float32)
    norm2_gain = jnp.clip(1.0 + 0.18 * jax.random.normal(key_list[6], (C,), jnp.float32), 0.1, 1.9)
    norm2_shift = noise(key_list[7], (C,), 0.5, 3.0, jnp.float32)
    conv2_weight = noise(key_list[8], (3, 3, C, C), (9 * C) ** -0.5, 0.109375)
    conv2_bias = noise(key_list[9], (C,), 0.5, 3.0, jnp.float32)
    return dict(latent=latent, norm1_gain=norm1_gain, norm1_shift=norm1_shift, conv1_weight=conv1_weight, conv1_bias=conv1_bias, emb_shift=emb_shift, norm2_gain=norm2_gain, norm2_shift=norm2_shift, conv2_weight=conv2_weight, conv2_bias=conv2_bias)


def sphere_pad(field):
    half = LON_COLS // 2
    north_row = jnp.roll(field[:, :1], -half, axis=2)
    south_row = jnp.roll(field[:, -1:], -half, axis=2)
    tall_field = jnp.concatenate([north_row, field, south_row], axis=1)
    return jnp.concatenate([tall_field[:, :, -1:], tall_field, tall_field[:, :, :1]], axis=2)

def group_stats(field):
    grouped = field.reshape(FRAMES, LAT_ROWS * LON_COLS, GROUPS, C // GROUPS)
    average = lax.optimization_barrier(jnp.mean(grouped, axis=(1, 3)))
    centered = grouped - average[:, None, :, None]
    variance = lax.optimization_barrier(jnp.mean(centered * centered, axis=(1, 3)))
    return (average, lax.rsqrt(variance + 1e-05))

def activate(field, average, inverse, norm_gain, norm_shift):
    per_mean = jnp.repeat(average, C // GROUPS, axis=1)[:, None, None, :]
    per_inverse = jnp.repeat(inverse, C // GROUPS, axis=1)[:, None, None, :]
    normed = (field - per_mean) * per_inverse * norm_gain + norm_shift
    return jax.nn.silu(normed).astype(jnp.bfloat16)

def convolve(padded, weight):
    return lax.conv_general_dilated(padded.astype(jnp.float32), weight.astype(jnp.float32), (1, 1), 'VALID', dimension_numbers=('NHWC', 'HWIO', 'NHWC'), precision=lax.Precision.HIGHEST)

def reference(latent, norm1_gain, norm1_shift, conv1_weight, conv1_bias, emb_shift, norm2_gain, norm2_shift, conv2_weight, conv2_bias):
    source = latent.astype(jnp.float32)
    average, inverse = group_stats(source)
    first_act = activate(source, average, inverse, norm1_gain, norm1_shift)
    hidden = convolve(sphere_pad(first_act), conv1_weight) + conv1_bias + emb_shift[:, None, None, :]
    hidden = hidden.astype(jnp.bfloat16)
    hidden_f = hidden.astype(jnp.float32)
    average, inverse = group_stats(hidden_f)
    second_act = activate(hidden_f, average, inverse, norm2_gain, norm2_shift)
    branch = convolve(sphere_pad(second_act), conv2_weight) + conv2_bias
    return (source + branch).astype(jnp.bfloat16)
```

```python
import functools

import jax
import jax.numpy as jnp
from jax import lax
from jax.experimental import pallas as pl
from jax.experimental.pallas import tpu as pltpu
from jax.sharding import PartitionSpec as P

GROUPS = 32
F = 4
T = 16
C = 320
KP = 384
F32 = jnp.float32
BF16 = jnp.bfloat16
MESH = pl.DeviceIdType.MESH


def kernel(
    n_lon,
    n_lat,
    x_hbm,
    g1_ref,
    s1_ref,
    w1_hbm,
    b1_ref,
    emb_ref,
    g2_ref,
    s2_ref,
    w2_hbm,
    b2_ref,
    o_ref,
    xv,
    hid,
    w1v,
    w2v,
    cols,
    stat,
    coef,
    msg,
    sums,
    rowbuf,
    colbuf,
    corbuf,
    colsend,
    corsend,
    x_sem,
    w_sem,
    ar_send,
    ar_recv,
    row_send,
    row_recv,
    col_send,
    col_recv,
    cor_send,
    cor_recv,
):
    n_y, n_z, half = n_lon // 4, n_lat // 2, n_lon // 2
    lon, lat = lax.axis_index("lon"), lax.axis_index("lat")
    y, x_hi, core = lon // 4, (lon // 2) % 2, lon % 2
    x_lo, z = lat // n_z, lat % n_z

    x_in = [pltpu.make_async_copy(x_hbm.at[f], xv.at[f], x_sem.at[f]) for f in range(F)]
    for cp in x_in:
        cp.start()
    w_in = []
    for k, (hbm, vm) in enumerate(((w1_hbm, w1v), (w2_hbm, w2v))):
        for a in range(3):
            for b in range(3):
                w_in.append(
                    pltpu.make_async_copy(
                        hbm.at[a, b], vm.at[a, pl.ds(b * KP, C)], w_sem.at[k, 3 * a + b]
                    )
                )
                w_in[-1].start()

    def flip(bit, on):
        return 1 - bit if on else bit

    stages = [[], [], []]
    for d in range(1, 8):
        h, c, l = flip(x_hi, d & 4), flip(core, d & 2), flip(x_lo, d & 1)
        stages[0].append((d, (y * 4 + h * 2 + c, l * n_z + z)))
    for d in range(1, n_y):
        stages[1].append((d, (((y + d) % n_y) * 4 + x_hi * 2 + core, lat)))
    for d in range(1, n_z):
        stages[2].append((d, (lon, x_lo * n_z + (z + d) % n_z)))

    at_pole = [(lat == 0).astype(jnp.int32), (lat == n_lat - 1).astype(jnp.int32)]
    row_lat = [lat - 1 + at_pole[0], lat + 1 - at_pole[1]]
    row_shift = [half * at_pole[0], half * at_pole[1]]
    row_side = [1 - at_pole[0], at_pole[1]]
    row_dev = [((lon + row_shift[v]) % n_lon, row_lat[v]) for v in range(2)]
    col_dev = [((lon + n_lon - 1) % n_lon, lat), ((lon + 1) % n_lon, lat)]
    cor_dev = [
        [((lon + row_shift[v] + n_lon + (2 * h - 1)) % n_lon, row_lat[v]) for h in range(2)]
        for v in range(2)
    ]

    barrier = pltpu.get_barrier_semaphore()
    greeted = [dev for stage in stages for _, dev in stage]
    greeted += row_dev + col_dev + cor_dev[0] + cor_dev[1]
    for dev in greeted:
        pl.semaphore_signal(barrier, inc=1, device_id=dev, device_id_type=MESH)

    for b in range(3):
        cols[:, :, pl.ds(b * KP + 256, 128)] = jnp.zeros((F, 18 * T, 128), BF16)
        for a in range(3):
            w1v[a, pl.ds(b * KP + C, KP - C), :] = jnp.zeros((KP - C, C), BF16)
            w2v[a, pl.ds(b * KP + C, KP - C), :] = jnp.zeros((KP - C, C), BF16)

    chan = lax.broadcasted_iota(jnp.int32, (C, 128), 0)
    group = lax.broadcasted_iota(jnp.int32, (C, 128), 1) % GROUPS
    per = C // GROUPS
    member = jnp.where((chan >= group * per) & (chan < group * per + per), 1.0, 0.0).astype(F32)
    row8 = lax.broadcasted_iota(jnp.int32, (8, 128), 0)
    lane8 = lax.broadcasted_iota(jnp.int32, (8, 128), 1)
    own_frame = (row8 % F) == (lane8 // GROUPS)

    def note_frame(f, v):
        flat = v.reshape(T * T, C)
        stat[pl.ds(f, 1), :] = jnp.sum(flat, axis=0, keepdims=True)
        stat[pl.ds(F + f, 1), :] = jnp.sum(flat * flat, axis=0, keepdims=True)
        for h, c in enumerate((0, T - 1)):
            column = v[:, c, :]
            colsend[h, f] = column.astype(BF16)
            for side, r in enumerate((0, T - 1)):
                corsend[side, h, pl.ds(f, 1), :] = column[r : r + 1, :]

    def exchange(p, src):
        sent = []
        for v, r in enumerate((0, T - 1)):
            sent.append(
                pltpu.make_async_remote_copy(
                    src_ref=src.at[:, r],
                    dst_ref=rowbuf.at[p, row_side[v]],
                    send_sem=row_send.at[p, v],
                    recv_sem=row_recv.at[p, row_side[v]],
                    device_id=row_dev[v],
                    device_id_type=MESH,
                )
            )
        for h in range(2):
            sent.append(
                pltpu.make_async_remote_copy(
                    src_ref=colsend.at[h],
                    dst_ref=colbuf.at[p, 1 - h],
                    send_sem=col_send.at[p, h],
                    recv_sem=col_recv.at[p, 1 - h],
                    device_id=col_dev[h],
                    device_id_type=MESH,
                )
            )
            for v in range(2):
                sent.append(
                    pltpu.make_async_remote_copy(
                        src_ref=corsend.at[v, h],
                        dst_ref=corbuf.at[p, row_side[v], 1 - h],
                        send_sem=cor_send.at[p, v, h],
                        recv_sem=cor_recv.at[p, row_side[v], 1 - h],
                        device_id=cor_dev[v][h],
                        device_id_type=MESH,
                    )
                )
        return sent

    def landed(p):
        for k in range(2):
            pltpu.make_async_copy(rowbuf.at[p, k], rowbuf.at[p, k], row_recv.at[p, k]).wait()
            pltpu.make_async_copy(colbuf.at[p, k], colbuf.at[p, k], col_recv.at[p, k]).wait()
            for h in range(2):
                pltpu.make_async_copy(
                    corbuf.at[p, k, h], corbuf.at[p, k, h], cor_recv.at[p, k, h]
                ).wait()

    def reduce_stats(p, between):
        per_group = jnp.dot(
            stat[...], member, precision=lax.Precision.HIGHEST, preferred_element_type=F32
        )
        picked = jnp.where(own_frame, per_group, 0.0)
        total = jnp.concatenate(
            [jnp.sum(picked[:F], axis=0, keepdims=True), jnp.sum(picked[F:], axis=0, keepdims=True)],
            axis=0,
        )
        sent = []
        for s, peers in enumerate(stages):
            msg[p, s] = total
            here = []
            for d, dev in peers:
                here.append(
                    pltpu.make_async_remote_copy(
                        src_ref=msg.at[p, s],
                        dst_ref=sums.at[p, s, d],
                        send_sem=ar_send.at[p, s, d],
                        recv_sem=ar_recv.at[p, s, d],
                        device_id=dev,
                        device_id_type=MESH,
                    )
                )
                here[-1].start()
            if s == 0:
                between()
            for cp in here:
                cp.wait_recv()
            for d, _ in peers:
                total = total + sums[p, s, d]
            sent += here
        for cp in sent:
            cp.wait_send()
        return total

    def coefficients(total, gain, shift):
        count = float(T * T * n_lon * n_lat * per)
        average = total[0:1] / count
        variance = total[1:2] / count - average * average
        inverse = lax.rsqrt(variance + 1e-05)
        both = jnp.concatenate(
            [jnp.broadcast_to(average, (F, 128)), jnp.broadcast_to(inverse, (F, 128))], axis=0
        )
        spread = lax.dot_general(
            jnp.where(own_frame, both, 0.0),
            member,
            (((1,), (1,)), ((), ())),
            precision=lax.Precision.HIGHEST,
            preferred_element_type=F32,
        )
        coef[0:8, :] = spread
        coef[8:9, :] = gain * 0.5
        coef[9:10, :] = shift * 0.5

    def convolve(p, f, src, wv):
        mean = coef[pl.ds(f, 1), :]
        scale = coef[pl.ds(F + f, 1), :] * coef[8:9, :]
        shift = coef[9:10, :]

        def act(v):
            lead = (1,) * (v.ndim - 2)
            m, k, s = (t.reshape(lead + (1, C)) for t in (mean, scale, shift))
            h = (v - m) * k + s
            return h + h * jnp.tanh(h)

        rows = jnp.concatenate([rowbuf[p, 0, f][None], src[f], rowbuf[p, 1, f][None]], axis=0)
        mid = act(rows.astype(F32))
        side = []
        for h in range(2):
            strip = jnp.concatenate(
                [
                    corbuf[p, 0, h, pl.ds(f, 1), :],
                    colbuf[p, h, f].astype(F32),
                    corbuf[p, 1, h, pl.ds(f, 1), :],
                ],
                axis=0,
            )
            side.append(act(strip)[:, None, :])
        west = jnp.concatenate([side[0], mid[:, : T - 1, :]], axis=1)
        east = jnp.concatenate([mid[:, 1:, :], side[1]], axis=1)
        for b, v in enumerate((west, mid, east)):
            cols[f, :, pl.ds(b * KP, C)] = v.astype(BF16).reshape(18 * T, C)
        acc = jnp.zeros((T * T, C), F32)
        for a in range(3):
            acc += jnp.dot(
                cols[f, pl.ds(a * T, T * T), :], wv[a], preferred_element_type=F32
            )
        return acc

    for f in range(F):
        x_in[f].wait()

    def first_notes(f, carry):
        note_frame(f, xv[f].astype(F32))
        return carry

    lax.fori_loop(0, F, first_notes, 0)
    pl.semaphore_wait(barrier, len(greeted))
    sent = exchange(0, xv)

    def start_all(copies):
        for cp in copies:
            cp.start()

    total = reduce_stats(0, lambda: start_all(sent))
    coefficients(total, g1_ref[...], s1_ref[...])
    landed(0)
    for cp in sent:
        cp.wait_send()
    for cp in w_in:
        cp.wait()

    def first_conv(f, carry):
        acc = convolve(0, f, xv, w1v)
        acc = acc + b1_ref[...] + emb_ref[pl.ds(f, 1), :]
        rounded = acc.astype(BF16).reshape(T, T, C)
        hid[f] = rounded
        note_frame(f, rounded.astype(F32))
        return carry

    lax.fori_loop(0, F, first_conv, 0)

    sent = exchange(1, hid)
    total = reduce_stats(1, lambda: start_all(sent))
    coefficients(total, g2_ref[...], s2_ref[...])
    landed(1)
    for cp in sent:
        cp.wait_send()

    def second_conv(f, carry):
        acc = convolve(1, f, hid, w2v)
        acc = acc + b2_ref[...] + xv[f].astype(F32).reshape(T * T, C)
        o_ref[f] = acc.astype(BF16).reshape(T, T, C)
        return carry

    lax.fori_loop(0, F, second_conv, 0)


def block(n_lon, n_lat, latent, g1, s1, w1, b1, emb, g2, s2, w2, b2):
    vm = pl.BlockSpec(memory_space=pltpu.VMEM)
    hbm = pl.BlockSpec(memory_space=pl.ANY)
    dma = pltpu.SemaphoreType.DMA
    row = lambda v: v.reshape(1, C)
    return pl.pallas_call(
        functools.partial(kernel, n_lon, n_lat),
        out_shape=jax.ShapeDtypeStruct((F, T, T, C), BF16),
        in_specs=[hbm, vm, vm, hbm, vm, vm, vm, vm, hbm, vm],
        out_specs=vm,
        scratch_shapes=[
            pltpu.VMEM((F, T, T, C), BF16),
            pltpu.VMEM((F, T, T, C), BF16),
            pltpu.VMEM((3, 3 * KP, C), BF16),
            pltpu.VMEM((3, 3 * KP, C), BF16),
            pltpu.VMEM((F, 18 * T, 3 * KP), BF16),
            pltpu.VMEM((8, C), F32),
            pltpu.VMEM((16, C), F32),
            pltpu.VMEM((2, 3, 2, 128), F32),
            pltpu.VMEM((2, 3, 8, 2, 128), F32),
            pltpu.VMEM((2, 2, F, T, C), BF16),
            pltpu.VMEM((2, 2, F, T, C), BF16),
            pltpu.VMEM((2, 2, 2, 8, C), F32),
            pltpu.VMEM((2, F, T, C), BF16),
            pltpu.VMEM((2, 2, 8, C), F32),
            dma((F,)),
            dma((2, 9)),
            dma((2, 3, 8)),
            dma((2, 3, 8)),
            dma((2, 2)),
            dma((2, 2)),
            dma((2, 2)),
            dma((2, 2)),
            dma((2, 2, 2)),
            dma((2, 2, 2)),
        ],
        compiler_params=pltpu.CompilerParams(collective_id=0, has_side_effects=True),
    )(latent, row(g1), row(s1), w1, row(b1), emb, row(g2), row(s2), w2, row(b2))


def solution(mesh):
    n_lon, n_lat = mesh.shape["lon"], mesh.shape["lat"]
    tile = P(None, "lat", "lon", None)
    return jax.shard_map(
        functools.partial(block, n_lon, n_lat),
        mesh=mesh,
        in_specs=(tile,) + (P(),) * 9,
        out_specs=tile,
        check_vma=False,
    )
```

```python
import functools

import jax
import jax.numpy as jnp
from jax import lax
from jax.experimental import pallas as pl
from jax.experimental.pallas import tpu as pltpu
from jax.sharding import PartitionSpec as P

GROUPS = 32
F = 4
T = 16
C = 320
LOW = 256
TAIL = C - LOW
K = 1024
F32 = jnp.float32
BF16 = jnp.bfloat16
MESH = pl.DeviceIdType.MESH


def kernel(
    n_lon,
    n_lat,
    x_hbm,
    g1_hbm,
    s1_hbm,
    w1_hbm,
    b1_hbm,
    emb_hbm,
    g2_hbm,
    s2_hbm,
    w2_hbm,
    b2_hbm,
    o_ref,
    xv,
    hid,
    wf,
    wt,
    cols,
    stat,
    coef,
    vecs,
    emb,
    msg,
    sums,
    halo,
    corner,
    colsend,
    corsend,
    x_sem,
    w_sem,
    v_sem,
    ar_send,
    ar_recv,
    halo_send,
    halo_recv,
    cor_send,
    cor_recv,
):
    n_y, n_z, half = n_lon // 4, n_lat // 2, n_lon // 2
    rem, div = lax.rem, lax.div
    lon, lat = lax.axis_index("lon"), lax.axis_index("lat")
    y, x_hi, core = div(lon, 4), rem(div(lon, 2), 2), rem(lon, 2)
    x_lo, z = div(lat, n_z), rem(lat, n_z)

    x_in = [pltpu.make_async_copy(x_hbm.at[f], xv.at[f], x_sem.at[f]) for f in range(F)]
    for cp in x_in:
        cp.start()

    def flip(bit, on):
        return 1 - bit if on else bit

    stages = [[], []]
    for d in range(1, 2 * n_y):
        to_y = rem(y + d // 2, n_y)
        stages[0].append((to_y * 4 + x_hi * 2 + flip(core, d % 2), lat))
    for d in range(1, 4 * n_z):
        to_z = rem(z + d // 4, n_z)
        to_lon = y * 4 + flip(x_hi, d & 1) * 2 + core
        stages[1].append((to_lon, flip(x_lo, d & 2) * n_z + to_z))

    at_pole = [(lat == 0).astype(jnp.int32), (lat == n_lat - 1).astype(jnp.int32)]
    row_lat = [lat - 1 + at_pole[0], lat + 1 - at_pole[1]]
    row_shift = [half * at_pole[0], half * at_pole[1]]
    row_side = [1 - at_pole[0], at_pole[1]]
    row_dev = [(rem(lon + row_shift[v], n_lon), row_lat[v]) for v in range(2)]
    col_dev = [(rem(lon + n_lon - 1, n_lon), lat), (rem(lon + 1, n_lon), lat)]
    cor_dev = [
        [(rem(lon + row_shift[v] + n_lon + (2 * h - 1), n_lon), row_lat[v]) for h in range(2)]
        for v in range(2)
    ]

    barrier = pltpu.get_barrier_semaphore()
    greeted = [dev for stage in stages for dev in stage]
    greeted += row_dev + col_dev + cor_dev[0] + cor_dev[1]
    for dev in greeted:
        pl.semaphore_signal(barrier, inc=1, device_id=dev, device_id_type=MESH)

    vec_in = [
        pltpu.make_async_copy(hbm, vecs.at[i], v_sem.at[i])
        for i, hbm in enumerate((g1_hbm, s1_hbm, b1_hbm, g2_hbm, s2_hbm, b2_hbm))
    ]
    vec_in.append(pltpu.make_async_copy(emb_hbm, emb, v_sem.at[6]))
    for cp in vec_in:
        cp.start()
    for k, hbm in enumerate((w1_hbm, w2_hbm)):
        for a in range(3):
            for b in range(3):
                pltpu.make_async_copy(
                    hbm.at[a, b, pl.ds(0, LOW)], wf.at[k, a, pl.ds(b * LOW, LOW)], w_sem.at[k]
                ).start()
                pltpu.make_async_copy(
                    hbm.at[a, b, pl.ds(LOW, TAIL)],
                    wf.at[k, a, pl.ds(3 * LOW + b * TAIL, TAIL)],
                    w_sem.at[k],
                ).start()

    per = C // GROUPS

    def member(shape, channel_dim):
        chan = lax.broadcasted_iota(jnp.int32, shape, channel_dim)
        group = lax.broadcasted_iota(jnp.int32, shape, 1 - channel_dim) & (GROUPS - 1)
        inside = (chan >= group * per) & (chan < group * per + per)
        return jnp.where(inside, 1.0, 0.0).astype(BF16)

    own_frame = (lax.broadcasted_iota(jnp.int32, (8, 128), 0) & (F - 1)) == (
        lax.broadcasted_iota(jnp.int32, (8, 128), 1) // GROUPS
    )

    def select(v, chosen):
        high = v.astype(BF16).astype(F32)
        middle = (v - high).astype(BF16).astype(F32)
        low = v - high - middle
        parts = jnp.concatenate([high, middle, low], axis=0).astype(BF16)
        out = jnp.dot(parts, chosen, preferred_element_type=F32)
        return out[0:8] + out[8:16] + out[16:24]

    def note_frame(f, v):
        flat = v.reshape(T * T, C)
        stat[pl.ds(f, 1), :] = jnp.sum(flat, axis=0, keepdims=True)
        stat[pl.ds(F + f, 1), :] = jnp.sum(flat * flat, axis=0, keepdims=True)
        for h, c in enumerate((0, T - 1)):
            column = v[:, c, :]
            colsend[h, f] = column.astype(BF16)
            for side, r in enumerate((0, T - 1)):
                corsend[side, h, pl.ds(f, 1), :] = column[r : r + 1, :]

    def remote(src, dst, send, recv, dev):
        pltpu.make_async_remote_copy(
            src_ref=src,
            dst_ref=dst,
            send_sem=send,
            recv_sem=recv,
            device_id=dev,
            device_id_type=MESH,
        ).start()

    def arrived(ref, sem):
        pltpu.make_async_copy(ref, ref, sem).wait()

    def exchange(p, src):
        for v, r in enumerate((0, T - 1)):
            remote(
                src.at[:, r], halo.at[p, row_side[v]], halo_send.at[p], halo_recv.at[p], row_dev[v]
            )
        for h in range(2):
            remote(
                colsend.at[h], halo.at[p, 3 - h], halo_send.at[p], halo_recv.at[p], col_dev[h]
            )
        for v in range(2):
            for h in range(2):
                remote(
                    corsend.at[v, h],
                    corner.at[p, row_side[v], 1 - h],
                    cor_send.at[p],
                    cor_recv.at[p],
                    cor_dev[v][h],
                )

    def reduce_stats(p, chosen, between):
        picked = jnp.where(own_frame, select(stat[...], chosen), 0.0)
        total = jnp.concatenate(
            [jnp.sum(picked[:F], axis=0, keepdims=True), jnp.sum(picked[F:], axis=0, keepdims=True)],
            axis=0,
        )
        for s, peers in enumerate(stages):
            msg[p, s] = total
            for i, dev in enumerate(peers):
                remote(msg.at[p, s], sums.at[p, s, i], ar_send.at[p, s], ar_recv.at[p, s], dev)
            if s == 0:
                between()
            n = len(peers)
            arrived(sums.at[p, s, pl.ds(0, n)], ar_recv.at[p, s])
            total = total + jnp.sum(sums[p, s, 0:n], axis=0)
        return total

    def sends_done(p):
        for s, peers in enumerate(stages):
            arrived(sums.at[p, s, pl.ds(0, len(peers))], ar_send.at[p, s])
        arrived(halo.at[p], halo_send.at[p])
        arrived(corner.at[p], cor_send.at[p])

    def coefficients(total, chosen, gain, shift):
        count = float(T * T * n_lon * n_lat * per)
        average = total[0:1] / count
        variance = total[1:2] / count - average * average
        inverse = lax.rsqrt(variance + 1e-05)
        both = jnp.concatenate(
            [jnp.broadcast_to(average, (F, 128)), jnp.broadcast_to(inverse, (F, 128))], axis=0
        )
        spread = select(jnp.where(own_frame, both, 0.0), chosen)
        coef[0:F, :] = spread[0:F]
        coef[F : 2 * F, :] = spread[F:] * (vecs[gain][None, :] * 0.5)
        coef[8:9, :] = vecs[shift][None, :] * 0.5

    def shifted(p, f, src):
        mean = coef[pl.ds(f, 1), :]
        scale = coef[pl.ds(F + f, 1), :]
        shift = coef[8:9, :]

        def act(v):
            lead = (1,) * (v.ndim - 2)
            m, k, s = (t.reshape(lead + (1, C)) for t in (mean, scale, shift))
            h = (v - m) * k + s
            return h + h * jnp.tanh(h)

        rows = jnp.concatenate([halo[p, 0, f][None], src[f], halo[p, 1, f][None]], axis=0)
        mid = act(rows.astype(F32))
        side = []
        for h in range(2):
            strip = jnp.concatenate(
                [
                    corner[p, 0, h, pl.ds(f, 1), :],
                    halo[p, 2 + h, f].astype(F32),
                    corner[p, 1, h, pl.ds(f, 1), :],
                ],
                axis=0,
            )
            side.append(act(strip)[:, None, :])
        west = jnp.concatenate([side[0], mid[:, : T - 1, :]], axis=1)
        east = jnp.concatenate([mid[:, 1:, :], side[1]], axis=1)
        taps = [v.reshape(18 * T, C) for v in (west, mid, east)]
        for b, v in enumerate(taps):
            cols[f, :, pl.ds(b * LOW, LOW)] = v[:, :LOW].astype(BF16)
        tails = [v[:, LOW:] for v in taps] + [jnp.zeros((18 * T, TAIL), F32)]
        for i in range(2):
            pair = jnp.concatenate(tails[2 * i : 2 * i + 2], axis=1)
            cols[f, :, pl.ds(3 * LOW + 128 * i, 128)] = pair.astype(BF16)

    def convolve(k, f):
        low = jnp.zeros((T * T, LOW), F32)
        for a in range(3):
            low += jnp.dot(
                cols[f, pl.ds(a * T, T * T), :], wf[k, a, :, 0:LOW], preferred_element_type=F32
            )
        side = jnp.dot(cols[f], wt[k], preferred_element_type=F32)
        tail = side[0 : T * T, 0:TAIL]
        tail = tail + side[T : T + T * T, TAIL : 2 * TAIL]
        tail = tail + side[2 * T : 2 * T + T * T, 2 * TAIL : 3 * TAIL]
        return jnp.concatenate([low, tail], axis=1)

    for f in range(F):
        x_in[f].wait()

    def first_notes(f, carry):
        note_frame(f, xv[f].astype(F32))
        return carry

    lax.fori_loop(0, F, first_notes, 0)
    to_groups = member((C, 128), 0)
    pl.semaphore_wait(barrier, len(greeted))

    def prepare():
        exchange(0, xv)
        for k in range(2):
            wf[k, :, pl.ds(3 * C, K - 3 * C), :] = jnp.zeros((3, K - 3 * C, C), BF16)
            arrived(wf.at[k, :, pl.ds(0, 3 * C)], w_sem.at[k])
            tails = [wf[k, a, :, LOW:C] for a in range(3)] + [jnp.zeros((K, TAIL), BF16)]
            for i in range(2):
                wt[k, :, pl.ds(128 * i, 128)] = jnp.concatenate(
                    tails[2 * i : 2 * i + 2], axis=1
                )
        for cp in vec_in:
            cp.wait()

    to_channels = member((128, C), 1)
    total = reduce_stats(0, to_groups, prepare)
    coefficients(total, to_channels, 0, 1)
    arrived(halo.at[0], halo_recv.at[0])
    arrived(corner.at[0], cor_recv.at[0])
    sends_done(0)

    def first_conv(f, carry):
        shifted(0, f, xv)
        acc = convolve(0, f) + (vecs[2][None, :] + emb[pl.ds(f, 1), :])
        rounded = acc.astype(BF16).reshape(T, T, C)
        hid[f] = rounded
        note_frame(f, rounded.astype(F32))
        return carry

    lax.fori_loop(0, F, first_conv, 0)

    total = reduce_stats(1, to_groups, lambda: exchange(1, hid))
    coefficients(total, to_channels, 3, 4)
    arrived(halo.at[1], halo_recv.at[1])
    arrived(corner.at[1], cor_recv.at[1])
    sends_done(1)

    def second_conv(f, carry):
        shifted(1, f, hid)
        acc = convolve(1, f) + vecs[5][None, :] + xv[f].astype(F32).reshape(T * T, C)
        o_ref[f] = acc.astype(BF16).reshape(T, T, C)
        return carry

    lax.fori_loop(0, F, second_conv, 0)


def block(n_lon, n_lat, *args):
    vm = pltpu.VMEM
    hbm = pl.BlockSpec(memory_space=pltpu.HBM)
    dma = pltpu.SemaphoreType.DMA
    n_peers = 2 * n_lat
    return pl.pallas_call(
        functools.partial(kernel, n_lon, n_lat),
        out_shape=jax.ShapeDtypeStruct((F, T, T, C), BF16),
        in_specs=[hbm] * 10,
        out_specs=pl.BlockSpec(memory_space=vm),
        scratch_shapes=[
            vm((F, T, T, C), BF16),
            vm((F, T, T, C), BF16),
            vm((2, 3, K, C), BF16),
            vm((2, K, 256), BF16),
            vm((F, 18 * T, K), BF16),
            vm((8, C), F32),
            vm((16, C), F32),
            vm((6, C), F32),
            vm((F, C), F32),
            vm((2, 2, 2, 128), F32),
            vm((2, 2, n_peers, 2, 128), F32),
            vm((2, 4, F, T, C), BF16),
            vm((2, 2, 2, 8, C), F32),
            vm((2, F, T, C), BF16),
            vm((2, 2, 8, C), F32),
            dma((F,)),
            dma((2,)),
            dma((7,)),
            dma((2, 2)),
            dma((2, 2)),
            dma((2,)),
            dma((2,)),
            dma((2,)),
            dma((2,)),
        ],
        compiler_params=pltpu.CompilerParams(collective_id=0, has_side_effects=True, vmem_limit_bytes=24 * 2**20),
    )(*[pltpu.with_memory_space_constraint(a, pltpu.HBM) for a in args])


def solution(mesh):
    n_lon, n_lat = mesh.shape["lon"], mesh.shape["lat"]
    tile = P(None, "lat", "lon", None)
    return jax.shard_map(
        functools.partial(block, n_lon, n_lat),
        mesh=mesh,
        in_specs=(tile,) + (P(),) * 9,
        out_specs=tile,
        check_vma=False,
    )
```

```python
import functools

import jax
import jax.numpy as jnp
from jax import lax
from jax.experimental import pallas as pl
from jax.experimental.pallas import tpu as pltpu
from jax.sharding import PartitionSpec as P

GROUPS = 32
F = 4
T = 16
C = 320
LOW = 256
TAIL = C - LOW
K = 1024
F32 = jnp.float32
BF16 = jnp.bfloat16
MESH = pl.DeviceIdType.MESH


def kernel(
    n_lon,
    n_lat,
    x_hbm,
    g1_hbm,
    s1_hbm,
    w1_hbm,
    b1_hbm,
    emb_hbm,
    g2_hbm,
    s2_hbm,
    w2_hbm,
    b2_hbm,
    o_ref,
    xv,
    hid,
    wf,
    wt,
    cols,
    stat,
    coef,
    vecs,
    emb,
    msg,
    msg2,
    sums,
    sums2,
    halo,
    corner,
    colsend,
    corsend,
    x_sem,
    w_sem,
    v_sem,
    ar_send,
    ar_recv,
    ar_send2,
    ar_recv2,
    halo_send,
    halo_recv,
    cor_send,
    cor_recv,
):
    n_y, n_z, half = n_lon // 4, n_lat // 2, n_lon // 2
    rem, div = lax.rem, lax.div
    lon, lat = lax.axis_index("lon"), lax.axis_index("lat")
    y, x_hi, core = div(lon, 4), rem(div(lon, 2), 2), rem(lon, 2)
    x_lo, z = div(lat, n_z), rem(lat, n_z)

    x_in = [pltpu.make_async_copy(x_hbm.at[f], xv.at[f], x_sem.at[f]) for f in range(F)]
    for cp in x_in:
        cp.start()

    def flip(bit, on):
        return 1 - bit if on else bit

    stages = [[], []]
    for d in range(1, 2 * n_y):
        to_y = rem(y + d // 2, n_y)
        stages[0].append((to_y * 4 + x_hi * 2 + flip(core, d % 2), lat))
    for d in range(1, 4 * n_z):
        to_z = rem(z + d // 4, n_z)
        to_lon = y * 4 + flip(x_hi, d & 1) * 2 + core
        stages[1].append((to_lon, flip(x_lo, d & 2) * n_z + to_z))

    at_pole = [(lat == 0).astype(jnp.int32), (lat == n_lat - 1).astype(jnp.int32)]
    row_lat = [lat - 1 + at_pole[0], lat + 1 - at_pole[1]]
    row_shift = [half * at_pole[0], half * at_pole[1]]
    row_side = [1 - at_pole[0], at_pole[1]]
    row_dev = [(rem(lon + row_shift[v], n_lon), row_lat[v]) for v in range(2)]
    col_dev = [(rem(lon + n_lon - 1, n_lon), lat), (rem(lon + 1, n_lon), lat)]
    cor_dev = [
        [(rem(lon + row_shift[v] + n_lon + (2 * h - 1), n_lon), row_lat[v]) for h in range(2)]
        for v in range(2)
    ]

    barrier = pltpu.get_barrier_semaphore()
    greeted = [dev for stage in stages for dev in stage]
    greeted += row_dev + col_dev + cor_dev[0] + cor_dev[1]
    for dev in greeted:
        pl.semaphore_signal(barrier, inc=1, device_id=dev, device_id_type=MESH)

    vec_in = [
        pltpu.make_async_copy(hbm, vecs.at[i], v_sem.at[i])
        for i, hbm in enumerate((g1_hbm, s1_hbm, b1_hbm, g2_hbm, s2_hbm, b2_hbm))
    ]
    vec_in.append(pltpu.make_async_copy(emb_hbm, emb, v_sem.at[6]))
    for cp in vec_in:
        cp.start()
    for k, hbm in enumerate((w1_hbm, w2_hbm)):
        for a in range(3):
            for b in range(3):
                pltpu.make_async_copy(
                    hbm.at[a, b, pl.ds(0, LOW)], wf.at[k, a, pl.ds(b * LOW, LOW)], w_sem.at[k]
                ).start()
                pltpu.make_async_copy(
                    hbm.at[a, b, pl.ds(LOW, TAIL)],
                    wf.at[k, a, pl.ds(3 * LOW + b * TAIL, TAIL)],
                    w_sem.at[k],
                ).start()

    per = C // GROUPS

    def member(shape, channel_dim):
        chan = lax.broadcasted_iota(jnp.int32, shape, channel_dim)
        group = lax.broadcasted_iota(jnp.int32, shape, 1 - channel_dim) & (GROUPS - 1)
        inside = (chan >= group * per) & (chan < group * per + per)
        return jnp.where(inside, 1.0, 0.0).astype(BF16)

    own_lanes = (lax.broadcasted_iota(jnp.int32, (8, 128), 0) & 3) == (
        lax.broadcasted_iota(jnp.int32, (8, 128), 1) // GROUPS
    )
    own_low_lanes = (lax.broadcasted_iota(jnp.int32, (8, 128), 0) & 1) == (
        lax.broadcasted_iota(jnp.int32, (8, 128), 1) // GROUPS
    )

    def select(v, chosen):
        high = v.astype(BF16).astype(F32)
        middle = (v - high).astype(BF16).astype(F32)
        low = v - high - middle
        parts = jnp.concatenate([high, middle, low], axis=0).astype(BF16)
        out = jnp.dot(parts, chosen, preferred_element_type=F32)
        return out[0:8] + out[8:16] + out[16:24]

    def note_frame(f, v):
        flat = v.reshape(T * T, C)
        row = div(f, 2) * 4 + rem(f, 2)
        stat[pl.ds(row, 1), :] = jnp.sum(flat, axis=0, keepdims=True)
        stat[pl.ds(row + 2, 1), :] = jnp.sum(flat * flat, axis=0, keepdims=True)
        for h, c in enumerate((0, T - 1)):
            column = v[:, c, :]
            colsend[h, f] = column.astype(BF16)
            for side, r in enumerate((0, T - 1)):
                corsend[side, h, pl.ds(f, 1), :] = column[r : r + 1, :]

    def remote(src, dst, send, recv, dev):
        pltpu.make_async_remote_copy(
            src_ref=src,
            dst_ref=dst,
            send_sem=send,
            recv_sem=recv,
            device_id=dev,
            device_id_type=MESH,
        ).start()

    def arrived(ref, sem):
        pltpu.make_async_copy(ref, ref, sem).wait()

    def exchange(p, src):
        for v, r in enumerate((0, T - 1)):
            remote(
                src.at[:, r], halo.at[p, row_side[v]], halo_send.at[p], halo_recv.at[p], row_dev[v]
            )
        for h in range(2):
            remote(
                colsend.at[h], halo.at[p, 3 - h], halo_send.at[p], halo_recv.at[p], col_dev[h]
            )
        for v in range(2):
            for h in range(2):
                remote(
                    corsend.at[v, h],
                    corner.at[p, row_side[v], 1 - h],
                    cor_send.at[p],
                    cor_recv.at[p],
                    cor_dev[v][h],
                )

    def local_sums(chosen):
        picked = jnp.where(own_lanes, select(stat[...], chosen), 0.0)
        return jnp.concatenate(
            [jnp.sum(picked[4 * h : 4 * h + 4], axis=0, keepdims=True) for h in range(2)], axis=0
        )

    def send_sums(s, total, out, into, send, recv):
        out[...] = total
        for i, dev in enumerate(stages[s]):
            remote(out, into.at[i], send, recv, dev)

    def take_sums(s, total, into, recv):
        n = len(stages[s])
        arrived(into.at[pl.ds(0, n)], recv)
        return total + jnp.sum(into[0:n], axis=0)

    def coefficients(h, total, chosen, gain, shift):
        count = float(T * T * n_lon * n_lat * per)
        average = total / count
        variance = pltpu.roll(average, 64, 1) - average * average
        inverse = lax.rsqrt(jnp.maximum(variance, 0.0) + 1e-05)
        both = jnp.concatenate(
            [jnp.broadcast_to(average, (2, 128)), jnp.broadcast_to(inverse, (2, 128))] * 2, axis=0
        )
        spread = select(jnp.where(own_low_lanes, both, 0.0), chosen)
        coef[4 * h : 4 * h + 2, :] = spread[0:2]
        coef[4 * h + 2 : 4 * h + 4, :] = spread[2:4] * (vecs[gain][None, :] * 0.5)
        coef[8:9, :] = vecs[shift][None, :] * 0.5

    def shifted(p, f, src):
        row = f // 2 * 4 + f % 2
        mean = coef[row : row + 1, :]
        scale = coef[row + 2 : row + 3, :]
        shift = coef[8:9, :]

        def act(v):
            lead = (1,) * (v.ndim - 2)
            m, k, s = (t.reshape(lead + (1, C)) for t in (mean, scale, shift))
            h = (v - m) * k + s
            return h + h * jnp.tanh(h)

        rows = jnp.concatenate([halo[p, 0, f][None], src[f], halo[p, 1, f][None]], axis=0)
        mid = act(rows.astype(F32))
        side = []
        for h in range(2):
            strip = jnp.concatenate(
                [
                    corner[p, 0, h, f : f + 1, :],
                    halo[p, 2 + h, f].astype(F32),
                    corner[p, 1, h, f : f + 1, :],
                ],
                axis=0,
            )
            side.append(act(strip)[:, None, :])
        west = jnp.concatenate([side[0], mid[:, : T - 1, :]], axis=1)
        east = jnp.concatenate([mid[:, 1:, :], side[1]], axis=1)
        taps = [v.reshape(18 * T, C) for v in (west, mid, east)]
        for b, v in enumerate(taps):
            cols[f, :, pl.ds(b * LOW, LOW)] = v[:, :LOW].astype(BF16)
        tails = [v[:, LOW:] for v in taps] + [jnp.zeros((18 * T, TAIL), F32)]
        for i in range(2):
            pair = jnp.concatenate(tails[2 * i : 2 * i + 2], axis=1)
            cols[f, :, pl.ds(3 * LOW + 128 * i, 128)] = pair.astype(BF16)

    def convolve(k, f):
        low = jnp.zeros((T * T, LOW), F32)
        for a in range(3):
            low += jnp.dot(
                cols[f, pl.ds(a * T, T * T), :], wf[k, a, :, 0:LOW], preferred_element_type=F32
            )
        side = jnp.dot(cols[f], wt[k], preferred_element_type=F32)
        tail = side[0 : T * T, 0:TAIL]
        tail = tail + side[T : T + T * T, TAIL : 2 * TAIL]
        tail = tail + side[2 * T : 2 * T + T * T, 2 * TAIL : 3 * TAIL]
        return jnp.concatenate([low, tail], axis=1)

    for f in range(F):
        x_in[f].wait()

    def first_notes(f, carry):
        note_frame(f, xv[f].astype(F32))
        return carry

    lax.fori_loop(0, F, first_notes, 0)
    to_groups = member((C, 128), 0)
    pl.semaphore_wait(barrier, len(greeted))

    def prepare():
        exchange(0, xv)
        for k in range(2):
            wf[k, :, pl.ds(3 * C, K - 3 * C), :] = jnp.zeros((3, K - 3 * C, C), BF16)
            arrived(wf.at[k, :, pl.ds(0, 3 * C)], w_sem.at[k])
            tails = [wf[k, a, :, LOW:C] for a in range(3)] + [jnp.zeros((K, TAIL), BF16)]
            for i in range(2):
                wt[k, :, pl.ds(128 * i, 128)] = jnp.concatenate(
                    tails[2 * i : 2 * i + 2], axis=1
                )
        for cp in vec_in:
            cp.wait()

    to_channels = member((128, C), 1)
    total = local_sums(to_groups)
    for s in range(2):
        send_sums(s, total, msg.at[s], sums.at[s], ar_send.at[s], ar_recv.at[s])
        if s == 0:
            prepare()
        total = take_sums(s, total, sums.at[s], ar_recv.at[s])
    for h in range(2):
        coefficients(h, total[h : h + 1], to_channels, 0, 1)
    arrived(halo.at[0], halo_recv.at[0])
    arrived(corner.at[0], cor_recv.at[0])
    for s, peers in enumerate(stages):
        arrived(sums.at[s, pl.ds(0, len(peers))], ar_send.at[s])
    arrived(halo.at[0], halo_send.at[0])
    arrived(corner.at[0], cor_send.at[0])

    def first_conv(f):
        acc = convolve(0, f) + (vecs[2][None, :] + emb[f : f + 1, :])
        rounded = acc.astype(BF16).reshape(T, T, C)
        hid[f] = rounded
        note_frame(f, rounded.astype(F32))

    def second_conv(f):
        acc = convolve(1, f) + vecs[5][None, :] + xv[f].astype(F32).reshape(T * T, C)
        o_ref[f] = acc.astype(BF16).reshape(T, T, C)

    totals = [None, None]
    shifted(0, 0, xv)
    for f in range(F):
        if f + 1 < F:
            shifted(0, f + 1, xv)
        first_conv(f)
        if f % 2 == 1:
            h = f // 2
            totals[h] = local_sums(to_groups)[h : h + 1]
            send_sums(
                0, totals[h], msg2.at[0, h], sums2.at[0, h], ar_send2.at[0, h], ar_recv2.at[0, h]
            )
    exchange(1, hid)
    for h in range(2):
        totals[h] = take_sums(0, totals[h], sums2.at[0, h], ar_recv2.at[0, h])
        send_sums(
            1, totals[h], msg2.at[1, h], sums2.at[1, h], ar_send2.at[1, h], ar_recv2.at[1, h]
        )
    arrived(halo.at[1], halo_recv.at[1])
    arrived(corner.at[1], cor_recv.at[1])
    for h in range(2):
        arrived(sums2.at[0, h, pl.ds(0, len(stages[0]))], ar_send2.at[0, h])
    arrived(halo.at[1], halo_send.at[1])
    arrived(corner.at[1], cor_send.at[1])
    for h in range(2):
        totals[h] = take_sums(1, totals[h], sums2.at[1, h], ar_recv2.at[1, h])
        coefficients(h, totals[h], to_channels, 3, 4)
        shifted(1, 2 * h, hid)
        shifted(1, 2 * h + 1, hid)
        second_conv(2 * h)
        second_conv(2 * h + 1)
    for h in range(2):
        arrived(sums2.at[1, h, pl.ds(0, len(stages[1]))], ar_send2.at[1, h])


def block(n_lon, n_lat, *args):
    vm = pltpu.VMEM
    hbm = pl.BlockSpec(memory_space=pltpu.HBM)
    dma = pltpu.SemaphoreType.DMA
    n_peers = 2 * n_lat
    return pl.pallas_call(
        functools.partial(kernel, n_lon, n_lat),
        out_shape=jax.ShapeDtypeStruct((F, T, T, C), BF16),
        in_specs=[hbm] * 10,
        out_specs=pl.BlockSpec(memory_space=vm),
        scratch_shapes=[
            vm((F, T, T, C), BF16),
            vm((F, T, T, C), BF16),
            vm((2, 3, K, C), BF16),
            vm((2, K, 256), BF16),
            vm((F, 18 * T, K), BF16),
            vm((8, C), F32),
            vm((16, C), F32),
            vm((6, C), F32),
            vm((F, C), F32),
            vm((2, 2, 128), F32),
            vm((2, 2, 1, 128), F32),
            vm((2, n_peers, 2, 128), F32),
            vm((2, 2, n_peers, 1, 128), F32),
            vm((2, 4, F, T, C), BF16),
            vm((2, 2, 2, 8, C), F32),
            vm((2, F, T, C), BF16),
            vm((2, 2, 8, C), F32),
            dma((F,)),
            dma((2,)),
            dma((7,)),
            dma((2,)),
            dma((2,)),
            dma((2, 2)),
            dma((2, 2)),
            dma((2,)),
            dma((2,)),
            dma((2,)),
            dma((2,)),
        ],
        compiler_params=pltpu.CompilerParams(collective_id=0, has_side_effects=True, vmem_limit_bytes=24 * 2**20),
    )(*[pltpu.with_memory_space_constraint(a, pltpu.HBM) for a in args])


def solution(mesh):
    n_lon, n_lat = mesh.shape["lon"], mesh.shape["lat"]
    tile = P(None, "lat", "lon", None)
    return jax.shard_map(
        functools.partial(block, n_lon, n_lat),
        mesh=mesh,
        in_specs=(tile,) + (P(),) * 9,
        out_specs=tile,
        check_vma=False,
    )
```

```python
import functools

import jax
import jax.numpy as jnp
from jax import lax
from jax.experimental import pallas as pl
from jax.experimental.pallas import tpu as pltpu
from jax.sharding import PartitionSpec as P

GROUPS = 32
F = 4
T = 16
C = 320
LOW = 256
TAIL = C - LOW
K = 1024
F32 = jnp.float32
BF16 = jnp.bfloat16
MESH = pl.DeviceIdType.MESH


def kernel(
    n_lon,
    n_lat,
    x_hbm,
    g1_hbm,
    s1_hbm,
    w1_hbm,
    b1_hbm,
    emb_hbm,
    g2_hbm,
    s2_hbm,
    w2_hbm,
    b2_hbm,
    o_ref,
    xv,
    hid,
    wf,
    wt,
    raw,
    cols,
    to_groups,
    to_lanes,
    wide,
    stat,
    coef,
    vecs,
    emb,
    msg,
    msg2,
    sums,
    sums2,
    halo,
    corner,
    colsend,
    corsend,
    x_sem,
    w_sem,
    v_sem,
    ar_send,
    ar_recv,
    ar_send2,
    ar_recv2,
    halo_send,
    halo_recv,
    cor_send,
    cor_recv,
):
    n_y, n_z, half = n_lon // 4, n_lat // 2, n_lon // 2
    rem, div = lax.rem, lax.div
    lon, lat = lax.axis_index("lon"), lax.axis_index("lat")
    y, x_hi, core = div(lon, 4), rem(div(lon, 2), 2), rem(lon, 2)
    x_lo, z = div(lat, n_z), rem(lat, n_z)

    x_in = [pltpu.make_async_copy(x_hbm.at[f], xv.at[f], x_sem.at[f]) for f in range(F)]
    for cp in x_in:
        cp.start()

    def flip(bit, on):
        return 1 - bit if on else bit

    def hops(step, n):
        return min(step, n - step)

    x_hops = (0, 2, 1, 1)
    stages = [[], []]
    for d in sorted(range(1, 2 * n_y), key=lambda d: -hops(d // 2, n_y)):
        to_y = rem(y + d // 2, n_y)
        stages[0].append((to_y * 4 + x_hi * 2 + flip(core, d % 2), lat))
    for d in sorted(range(1, 4 * n_z), key=lambda d: -hops(d // 4, n_z) - x_hops[d % 4]):
        to_z = rem(z + d // 4, n_z)
        to_lon = y * 4 + flip(x_hi, d & 1) * 2 + core
        stages[1].append((to_lon, flip(x_lo, d & 2) * n_z + to_z))

    at_pole = [(lat == 0).astype(jnp.int32), (lat == n_lat - 1).astype(jnp.int32)]
    row_lat = [lat - 1 + at_pole[0], lat + 1 - at_pole[1]]
    row_shift = [half * at_pole[0], half * at_pole[1]]
    row_side = [1 - at_pole[0], at_pole[1]]
    row_dev = [(rem(lon + row_shift[v], n_lon), row_lat[v]) for v in range(2)]
    col_dev = [(rem(lon + n_lon - 1, n_lon), lat), (rem(lon + 1, n_lon), lat)]
    cor_dev = [
        [(rem(lon + row_shift[v] + n_lon + (2 * h - 1), n_lon), row_lat[v]) for h in range(2)]
        for v in range(2)
    ]

    barrier = pltpu.get_barrier_semaphore()
    greeted = stages[1] + stages[0] + cor_dev[0] + cor_dev[1] + row_dev + col_dev
    for dev in greeted:
        pl.semaphore_signal(barrier, inc=1, device_id=dev, device_id_type=MESH)

    vec_in = [
        pltpu.make_async_copy(hbm, vecs.at[i], v_sem.at[i])
        for i, hbm in enumerate((g1_hbm, s1_hbm, b1_hbm, g2_hbm, s2_hbm, b2_hbm))
    ]
    vec_in.append(pltpu.make_async_copy(emb_hbm, emb, v_sem.at[6]))
    for cp in vec_in:
        cp.start()
    for k, hbm in enumerate((w1_hbm, w2_hbm)):
        for a in range(3):
            for b in range(3):
                pltpu.make_async_copy(
                    hbm.at[a, b, pl.ds(0, LOW)], wf.at[k, a, pl.ds(b * LOW, LOW)], w_sem.at[k]
                ).start()
                pltpu.make_async_copy(
                    hbm.at[a, b, pl.ds(LOW, TAIL)],
                    wf.at[k, a, pl.ds(3 * LOW + b * TAIL, TAIL)],
                    w_sem.at[k],
                ).start()

    per = C // GROUPS

    def member(chan, group):
        inside = (chan >= group * per) & (chan < group * per + per)
        return jnp.where(inside, 1.0, 0.0).astype(BF16)

    def iota(shape, dim):
        return lax.broadcasted_iota(jnp.int32, shape, dim)

    own_lanes = (lax.broadcasted_iota(jnp.int32, (8, 128), 0) & 3) == (
        lax.broadcasted_iota(jnp.int32, (8, 128), 1) // GROUPS
    )
    own_low_lanes = (lax.broadcasted_iota(jnp.int32, (8, 128), 0) & 1) == (
        lax.broadcasted_iota(jnp.int32, (8, 128), 1) // GROUPS
    )

    def select(v, chosen):
        high = v.astype(BF16).astype(F32)
        middle = (v - high).astype(BF16).astype(F32)
        low = v - high - middle
        parts = jnp.concatenate([high, middle, low], axis=0).astype(BF16)
        out = jnp.dot(parts, chosen, preferred_element_type=F32)
        return out[0:8] + out[8:16] + out[16:24]

    def note_frame(f, v):
        flat = v.reshape(T * T, C)
        row = div(f, 2) * 4 + rem(f, 2)
        stat[pl.ds(row, 1), :] = jnp.sum(flat, axis=0, keepdims=True)
        stat[pl.ds(row + 2, 1), :] = jnp.sum(flat * flat, axis=0, keepdims=True)

    def note_edges(f, v):
        for h, c in enumerate((0, T - 1)):
            column = v[:, c, :]
            colsend[h, f] = column.astype(BF16)
            for side, r in enumerate((0, T - 1)):
                corsend[side, h, pl.ds(f, 1), :] = column[r : r + 1, :]

    def remote(src, dst, send, recv, dev):
        pltpu.make_async_remote_copy(
            src_ref=src,
            dst_ref=dst,
            send_sem=send,
            recv_sem=recv,
            device_id=dev,
            device_id_type=MESH,
        ).start()

    def arrived(ref, sem):
        pltpu.make_async_copy(ref, ref, sem).wait()

    def exchange(p, src):
        for v, r in enumerate((0, T - 1)):
            remote(
                src.at[:, r], halo.at[p, row_side[v]], halo_send.at[p], halo_recv.at[p], row_dev[v]
            )

        def edges(f, carry):
            note_edges(f, src[f].astype(F32))
            return carry

        lax.fori_loop(0, F, edges, 0)
        for v in range(2):
            for h in range(2):
                remote(
                    corsend.at[v, h],
                    corner.at[p, row_side[v], 1 - h],
                    cor_send.at[p],
                    cor_recv.at[p],
                    cor_dev[v][h],
                )
        for h in range(2):
            remote(colsend.at[h], halo.at[p, 3 - h], halo_send.at[p], halo_recv.at[p], col_dev[h])

    def local_sums():
        picked = jnp.where(own_lanes, select(stat[...], to_groups[...]), 0.0)
        return jnp.concatenate(
            [jnp.sum(picked[4 * h : 4 * h + 4], axis=0, keepdims=True) for h in range(2)], axis=0
        )

    def send_sums(s, total, out, into, send, recv):
        out[...] = total
        for i, dev in enumerate(stages[s]):
            remote(out, into.at[i], send, recv, dev)

    def take_sums(s, total, into, recv):
        n = len(stages[s])
        arrived(into.at[pl.ds(0, n)], recv)
        return total + jnp.sum(into[0:n], axis=0)

    def coefficients(p, h, total):
        count = float(T * T * n_lon * n_lat * per)
        average = total / count
        variance = pltpu.roll(average, 64, 1) - average * average
        inverse = lax.rsqrt(jnp.maximum(variance, 0.0) + 1e-05)
        both = jnp.concatenate(
            [jnp.broadcast_to(average, (2, 128)), jnp.broadcast_to(inverse, (2, 128))] * 2, axis=0
        )
        spread = select(jnp.where(own_low_lanes, both, 0.0), to_lanes[...])
        coef[4 * h : 4 * h + 2, :] = spread[0:2]
        coef[4 * h + 2 : 4 * h + 4, :] = spread[2:4] * wide[2 * p : 2 * p + 1, :]

    def widen(v):
        return jnp.concatenate(
            [v[:, :LOW]] * 3 + [v[:, LOW:]] * 3 + [jnp.zeros((1, K - 3 * C), F32)], axis=1
        )

    def arrange(p, src):
        def one(f, carry):
            rows = jnp.concatenate([halo[p, 0, f][None], src[f], halo[p, 1, f][None]], axis=0)
            mid = rows.astype(F32)
            side = []
            for h in range(2):
                strip = jnp.concatenate(
                    [
                        corner[p, 0, h, pl.ds(f, 1), :],
                        halo[p, 2 + h, f].astype(F32),
                        corner[p, 1, h, pl.ds(f, 1), :],
                    ],
                    axis=0,
                )
                side.append(strip[:, None, :])
            west = jnp.concatenate([side[0], mid[:, : T - 1, :]], axis=1)
            east = jnp.concatenate([mid[:, 1:, :], side[1]], axis=1)
            taps = [v.reshape(18 * T, C) for v in (west, mid, east)]
            for b, v in enumerate(taps):
                raw[f, :, pl.ds(b * LOW, LOW)] = v[:, :LOW].astype(BF16)
            tails = [v[:, LOW:] for v in taps] + [jnp.zeros((18 * T, TAIL), F32)]
            for i in range(2):
                pair = jnp.concatenate(tails[2 * i : 2 * i + 2], axis=1)
                raw[f, :, pl.ds(3 * LOW + 128 * i, 128)] = pair.astype(BF16)
            return carry

        lax.fori_loop(0, F, one, 0)

    def activate(p, f):
        row = f // 2 * 4 + f % 2
        for i in range(K // LOW):
            lanes = pl.ds(i * LOW, LOW)
            v = raw[f, :, lanes].astype(F32)
            h = (v - coef[row : row + 1, lanes]) * coef[row + 2 : row + 3, lanes]
            h = h + wide[2 * p + 1 : 2 * p + 2, lanes]
            cols[f, :, lanes] = (h + h * jnp.tanh(h)).astype(BF16)

    def convolve(k, f):
        low = jnp.zeros((T * T, LOW), F32)
        for a in range(3):
            low += jnp.dot(
                cols[f, pl.ds(a * T, T * T), :], wf[k, a, :, 0:LOW], preferred_element_type=F32
            )
        side = jnp.dot(cols[f], wt[k], preferred_element_type=F32)
        tail = side[0 : T * T, 0:TAIL]
        tail = tail + side[T : T + T * T, TAIL : 2 * TAIL]
        tail = tail + side[2 * T : 2 * T + T * T, 2 * TAIL : 3 * TAIL]
        return jnp.concatenate([low, tail], axis=1)

    for f in range(F):
        x_in[f].wait()

    def first_notes(f, carry):
        note_frame(f, xv[f].astype(F32))
        return carry

    lax.fori_loop(0, F, first_notes, 0)
    to_groups[...] = member(iota((C, 128), 0), iota((C, 128), 1) & (GROUPS - 1))
    pl.semaphore_wait(barrier, len(greeted))

    def prepare():
        exchange(0, xv)
        lane = iota((128, K), 1)
        chan = jnp.where(lane < 3 * LOW, lane & (LOW - 1), LOW + (lane & (TAIL - 1)))
        chan = jnp.where(lane < 3 * C, chan, -1)
        to_lanes[...] = member(chan, iota((128, K), 0) & (GROUPS - 1))
        for k in range(2):
            wf[k, :, pl.ds(3 * C, K - 3 * C), :] = jnp.zeros((3, K - 3 * C, C), BF16)
            arrived(wf.at[k, :, pl.ds(0, 3 * C)], w_sem.at[k])
            tails = [wf[k, a, :, LOW:C] for a in range(3)] + [jnp.zeros((K, TAIL), BF16)]
            for i in range(2):
                wt[k, :, pl.ds(128 * i, 128)] = jnp.concatenate(
                    tails[2 * i : 2 * i + 2], axis=1
                )
        for cp in vec_in:
            cp.wait()
        for row, i in enumerate((0, 1, 3, 4)):
            wide[row : row + 1, :] = widen(vecs[i : i + 1, :] * 0.5)

    total = local_sums()
    for s in range(2):
        send_sums(s, total, msg.at[s], sums.at[s], ar_send.at[s], ar_recv.at[s])
        if s == 0:
            prepare()
        else:
            arrived(halo.at[0], halo_recv.at[0])
            arrived(corner.at[0], cor_recv.at[0])
            arrange(0, xv)
        total = take_sums(s, total, sums.at[s], ar_recv.at[s])
    for h in range(2):
        coefficients(0, h, total[h : h + 1])
    for s, peers in enumerate(stages):
        arrived(sums.at[s, pl.ds(0, len(peers))], ar_send.at[s])
    arrived(halo.at[0], halo_send.at[0])
    arrived(corner.at[0], cor_send.at[0])

    totals = [None, None]
    activate(0, 0)
    for f in range(F):
        acc = convolve(0, f)
        if f + 1 < F:
            activate(0, f + 1)
        acc = acc + (vecs[2:3, :] + emb[f : f + 1, :])
        rounded = acc.astype(BF16).reshape(T, T, C)
        hid[f] = rounded
        note_frame(f, rounded.astype(F32))
        if f % 2 == 1:
            h = f // 2
            totals[h] = local_sums()[h : h + 1]
            send_sums(
                0, totals[h], msg2.at[0, h], sums2.at[0, h], ar_send2.at[0, h], ar_recv2.at[0, h]
            )
    exchange(1, hid)
    for h in range(2):
        totals[h] = take_sums(0, totals[h], sums2.at[0, h], ar_recv2.at[0, h])
        send_sums(
            1, totals[h], msg2.at[1, h], sums2.at[1, h], ar_send2.at[1, h], ar_recv2.at[1, h]
        )
    arrived(halo.at[1], halo_recv.at[1])
    arrived(corner.at[1], cor_recv.at[1])
    arrange(1, hid)
    for h in range(2):
        arrived(sums2.at[0, h, pl.ds(0, len(stages[0]))], ar_send2.at[0, h])
    arrived(halo.at[1], halo_send.at[1])
    arrived(corner.at[1], cor_send.at[1])

    for h in range(2):
        totals[h] = take_sums(1, totals[h], sums2.at[1, h], ar_recv2.at[1, h])
        coefficients(1, h, totals[h])
        activate(1, 2 * h)
        for f in (2 * h, 2 * h + 1):
            acc = convolve(1, f)
            if f == 2 * h:
                activate(1, f + 1)
            acc = acc + vecs[5:6, :] + xv[f].astype(F32).reshape(T * T, C)
            o_ref[f] = acc.astype(BF16).reshape(T, T, C)
    for h in range(2):
        arrived(sums2.at[1, h, pl.ds(0, len(stages[1]))], ar_send2.at[1, h])


def block(n_lon, n_lat, *args):
    vm = pltpu.VMEM
    hbm = pl.BlockSpec(memory_space=pltpu.HBM)
    dma = pltpu.SemaphoreType.DMA
    n_peers = 2 * n_lat
    return pl.pallas_call(
        functools.partial(kernel, n_lon, n_lat),
        out_shape=jax.ShapeDtypeStruct((F, T, T, C), BF16),
        in_specs=[hbm] * 10,
        out_specs=pl.BlockSpec(memory_space=vm),
        scratch_shapes=[
            vm((F, T, T, C), BF16),
            vm((F, T, T, C), BF16),
            vm((2, 3, K, C), BF16),
            vm((2, K, 256), BF16),
            vm((F, 18 * T, K), BF16),
            vm((F, 18 * T, K), BF16),
            vm((C, 128), BF16),
            vm((128, K), BF16),
            vm((4, K), F32),
            vm((8, C), F32),
            vm((8, K), F32),
            vm((6, C), F32),
            vm((F, C), F32),
            vm((2, 2, 128), F32),
            vm((2, 2, 1, 128), F32),
            vm((2, n_peers, 2, 128), F32),
            vm((2, 2, n_peers, 1, 128), F32),
            vm((2, 4, F, T, C), BF16),
            vm((2, 2, 2, F, C), F32),
            vm((2, F, T, C), BF16),
            vm((2, 2, F, C), F32),
            dma((F,)),
            dma((2,)),
            dma((7,)),
            dma((2,)),
            dma((2,)),
            dma((2, 2)),
            dma((2, 2)),
            dma((2,)),
            dma((2,)),
            dma((2,)),
            dma((2,)),
        ],
        compiler_params=pltpu.CompilerParams(collective_id=0, has_side_effects=True, vmem_limit_bytes=24 * 2**20),
    )(*[pltpu.with_memory_space_constraint(a, pltpu.HBM) for a in args])


def solution(mesh):
    n_lon, n_lat = mesh.shape["lon"], mesh.shape["lat"]
    tile = P(None, "lat", "lon", None)
    return jax.shard_map(
        functools.partial(block, n_lon, n_lat),
        mesh=mesh,
        in_specs=(tile,) + (P(),) * 9,
        out_specs=tile,
        check_vma=False,
    )
```

```python
import functools

import jax
import jax.numpy as jnp
from jax import lax
from jax.experimental import pallas as pl
from jax.experimental.pallas import tpu as pltpu
from jax.sharding import PartitionSpec as P

GROUPS = 32
F = 4
T = 16
C = 320
LOW = 256
TAIL = C - LOW
K = 1024
F32 = jnp.float32
BF16 = jnp.bfloat16
MESH = pl.DeviceIdType.MESH


def kernel(
    n_lon,
    n_lat,
    x_hbm,
    g1_hbm,
    s1_hbm,
    w1_hbm,
    b1_hbm,
    emb_hbm,
    g2_hbm,
    s2_hbm,
    w2_hbm,
    b2_hbm,
    o_ref,
    xv,
    hid,
    wf,
    wt,
    raw,
    cols,
    to_groups,
    to_lanes,
    wide,
    stat,
    coef,
    vecs,
    emb,
    msg,
    msg2,
    sums,
    sums2,
    halo,
    corner,
    colsend,
    corsend,
    x_sem,
    w_sem,
    v_sem,
    ar_send,
    ar_recv,
    ar_send2,
    ar_recv2,
    halo_send,
    halo_recv,
    cor_send,
    cor_recv,
):
    n_y, n_z, half = n_lon // 4, n_lat // 2, n_lon // 2
    rem, div = lax.rem, lax.div
    lon, lat = lax.axis_index("lon"), lax.axis_index("lat")
    y, x_hi, core = div(lon, 4), rem(div(lon, 2), 2), rem(lon, 2)
    x_lo, z = div(lat, n_z), rem(lat, n_z)

    def flip(bit, on):
        return 1 - bit if on else bit

    def hops(step, n):
        return min(step, n - step)

    x_hops = (0, 2, 1, 1)
    stages = [[], []]
    for d in sorted(range(1, 2 * n_y), key=lambda d: -hops(d // 2, n_y)):
        to_y = rem(y + d // 2, n_y)
        stages[0].append((to_y * 4 + x_hi * 2 + flip(core, d % 2), lat))
    for d in sorted(range(1, 4 * n_z), key=lambda d: -hops(d // 4, n_z) - x_hops[d % 4]):
        to_z = rem(z + d // 4, n_z)
        to_lon = y * 4 + flip(x_hi, d & 1) * 2 + core
        stages[1].append((to_lon, flip(x_lo, d & 2) * n_z + to_z))

    at_pole = [(lat == 0).astype(jnp.int32), (lat == n_lat - 1).astype(jnp.int32)]
    row_lat = [lat - 1 + at_pole[0], lat + 1 - at_pole[1]]
    row_shift = [half * at_pole[0], half * at_pole[1]]
    row_side = [1 - at_pole[0], at_pole[1]]
    row_dev = [(rem(lon + row_shift[v], n_lon), row_lat[v]) for v in range(2)]
    col_dev = [(rem(lon + n_lon - 1, n_lon), lat), (rem(lon + 1, n_lon), lat)]
    cor_dev = [
        [(rem(lon + row_shift[v] + n_lon + (2 * h - 1), n_lon), row_lat[v]) for h in range(2)]
        for v in range(2)
    ]

    greeted = stages[1] + stages[0] + cor_dev[0] + cor_dev[1] + row_dev + col_dev
    barrier = pltpu.get_barrier_semaphore()
    for dev in greeted:
        pl.semaphore_signal(barrier, inc=1, device_id=dev, device_id_type=MESH)
    for f in range(F):
        pltpu.make_async_copy(x_hbm.at[f], xv.at[f], x_sem).start()

    vec_in = [
        pltpu.make_async_copy(hbm, vecs.at[i, 0], v_sem.at[0])
        for i, hbm in enumerate((g1_hbm, s1_hbm, b1_hbm, g2_hbm, s2_hbm, b2_hbm))
    ]
    vec_in.append(pltpu.make_async_copy(emb_hbm, emb, v_sem.at[1]))
    for cp in vec_in:
        cp.start()
    for k, hbm in enumerate((w1_hbm, w2_hbm)):
        for a in range(3):
            for b in range(3):
                pltpu.make_async_copy(
                    hbm.at[a, b, pl.ds(0, LOW)], wf.at[k, a, pl.ds(b * LOW, LOW)], w_sem.at[k]
                ).start()
                pltpu.make_async_copy(
                    hbm.at[a, b, pl.ds(LOW, TAIL)],
                    wf.at[k, a, pl.ds(3 * LOW + b * TAIL, TAIL)],
                    w_sem.at[k],
                ).start()

    per = C // GROUPS

    def member(chan, group):
        inside = (chan >= group * per) & (chan < group * per + per)
        return jnp.where(inside, 1.0, 0.0).astype(BF16)

    def iota(shape, dim):
        return lax.broadcasted_iota(jnp.int32, shape, dim)

    own_lanes = (lax.broadcasted_iota(jnp.int32, (8, 128), 0) & 3) == (
        lax.broadcasted_iota(jnp.int32, (8, 128), 1) // GROUPS
    )
    own_low_lanes = (lax.broadcasted_iota(jnp.int32, (8, 128), 0) & 1) == (
        lax.broadcasted_iota(jnp.int32, (8, 128), 1) // GROUPS
    )

    def select(v, chosen):
        high = v.astype(BF16).astype(F32)
        middle = (v - high).astype(BF16).astype(F32)
        low = v - high - middle
        parts = jnp.concatenate([high, middle, low], axis=0).astype(BF16)
        out = jnp.dot(parts, chosen, preferred_element_type=F32)
        return out[0:8] + out[8:16] + out[16:24]

    def note_frame(f, v):
        flat = v.reshape(T * T, C)
        row = div(f, 2) * 4 + rem(f, 2)
        stat[pl.ds(row, 1), :] = jnp.sum(flat, axis=0, keepdims=True)
        stat[pl.ds(row + 2, 1), :] = jnp.sum(flat * flat, axis=0, keepdims=True)

    def note_edges(f, v):
        for h, c in enumerate((0, T - 1)):
            column = v[:, c, :]
            colsend[h, f] = column.astype(BF16)
            for side, r in enumerate((0, T - 1)):
                corsend[side, h, pl.ds(f, 1), :] = column[r : r + 1, :]

    def remote(src, dst, send, recv, dev):
        pltpu.make_async_remote_copy(
            src_ref=src,
            dst_ref=dst,
            send_sem=send,
            recv_sem=recv,
            device_id=dev,
            device_id_type=MESH,
        ).start()

    def arrived(ref, sem):
        pltpu.make_async_copy(ref, ref, sem).wait()

    def exchange(p, src):
        for v, r in enumerate((0, T - 1)):
            remote(
                src.at[:, r], halo.at[p, row_side[v]], halo_send, halo_recv.at[p], row_dev[v]
            )

        def edges(f, carry):
            note_edges(f, src[f].astype(F32))
            return carry

        lax.fori_loop(0, F, edges, 0)
        for v in range(2):
            for h in range(2):
                remote(
                    corsend.at[v, h],
                    corner.at[p, row_side[v], 1 - h],
                    cor_send,
                    cor_recv.at[p],
                    cor_dev[v][h],
                )
        for h in range(2):
            remote(colsend.at[h], halo.at[p, 3 - h], halo_send, halo_recv.at[p], col_dev[h])

    def local_sums():
        picked = jnp.where(own_lanes, select(stat[...], to_groups[...]), 0.0)
        return jnp.concatenate(
            [jnp.sum(picked[4 * h : 4 * h + 4], axis=0, keepdims=True) for h in range(2)], axis=0
        )

    def slots(s, h, n_halves):
        n = [len(stage) for stage in stages]
        return pl.ds(n[0] * h if s == 0 else n[0] * n_halves + n[1] * h, n[s])

    def send_sums(s, total, out, into, send, recv):
        out[...] = total
        for i, dev in enumerate(stages[s]):
            remote(out, into.at[i], send, recv, dev)

    def take_sums(total, into, recv):
        arrived(into, recv)
        return total + jnp.sum(into[...], axis=0)

    def coefficients(p, h, total):
        count = float(T * T * n_lon * n_lat * per)
        average = total / count
        variance = pltpu.roll(average, 64, 1) - average * average
        inverse = lax.rsqrt(jnp.maximum(variance, 0.0) + 1e-05)
        both = jnp.concatenate(
            [jnp.broadcast_to(average, (2, 128)), jnp.broadcast_to(inverse, (2, 128))] * 2, axis=0
        )
        spread = select(jnp.where(own_low_lanes, both, 0.0), to_lanes[...])
        scale = spread[2:4] * wide[2 * p : 2 * p + 1, :]
        coef[4 * h : 4 * h + 2, :] = wide[2 * p + 1 : 2 * p + 2, :] - spread[0:2] * scale
        coef[4 * h + 2 : 4 * h + 4, :] = scale

    def widen(v):
        return jnp.concatenate(
            [v[:, :LOW]] * 3 + [v[:, LOW:]] * 3 + [jnp.zeros((1, K - 3 * C), F32)], axis=1
        )

    def arrange(p, src):
        def one(f, carry):
            rows = jnp.concatenate([halo[p, 0, f][None], src[f], halo[p, 1, f][None]], axis=0)
            mid = rows.astype(F32)
            side = []
            for h in range(2):
                strip = jnp.concatenate(
                    [
                        corner[p, 0, h, pl.ds(f, 1), :],
                        halo[p, 2 + h, f].astype(F32),
                        corner[p, 1, h, pl.ds(f, 1), :],
                    ],
                    axis=0,
                )
                side.append(strip[:, None, :])
            west = jnp.concatenate([side[0], mid[:, : T - 1, :]], axis=1)
            east = jnp.concatenate([mid[:, 1:, :], side[1]], axis=1)
            taps = [v.reshape(18 * T, C) for v in (west, mid, east)]
            for b, v in enumerate(taps):
                raw[f, :, pl.ds(b * LOW, LOW)] = v[:, :LOW].astype(BF16)
            tails = [v[:, LOW:] for v in taps] + [jnp.zeros((18 * T, TAIL), F32)]
            for i in range(2):
                pair = jnp.concatenate(tails[2 * i : 2 * i + 2], axis=1)
                raw[f, :, pl.ds(3 * LOW + 128 * i, 128)] = pair.astype(BF16)
            return carry

        lax.fori_loop(0, F, one, 0)

    def activate(f):
        row = f // 2 * 4 + f % 2
        for i in range(K // LOW):
            lanes = pl.ds(i * LOW, LOW)
            v = raw[f, :, lanes].astype(F32)
            h = v * coef[row + 2 : row + 3, lanes] + coef[row : row + 1, lanes]
            cols[f, :, lanes] = (h + h * jnp.tanh(h)).astype(BF16)

    def convolve(k, f):
        low = jnp.zeros((T * T, LOW), F32)
        for a in range(3):
            low += jnp.dot(
                cols[f, pl.ds(a * T, T * T), :], wf[k, a, :, 0:LOW], preferred_element_type=F32
            )
        side = jnp.dot(cols[f], wt[k], preferred_element_type=F32)
        tail = side[0 : T * T, 0:TAIL]
        tail = tail + side[T : T + T * T, TAIL : 2 * TAIL]
        tail = tail + side[2 * T : 2 * T + T * T, 2 * TAIL : 3 * TAIL]
        return jnp.concatenate([low, tail], axis=1)

    arrived(xv, x_sem)

    def first_notes(f, carry):
        note_frame(f, xv[f].astype(F32))
        return carry

    lax.fori_loop(0, F, first_notes, 0)
    to_groups[...] = member(iota((C, 128), 0), iota((C, 128), 1) & (GROUPS - 1))
    total = local_sums()
    pl.semaphore_wait(barrier, len(greeted))

    def prepare():
        exchange(0, xv)
        lane = iota((128, K), 1)
        chan = jnp.where(lane < 3 * LOW, lane & (LOW - 1), LOW + (lane & (TAIL - 1)))
        chan = jnp.where(lane < 3 * C, chan, -1)
        to_lanes[...] = member(chan, iota((128, K), 0) & (GROUPS - 1))
        for k in range(2):
            wf[k, :, pl.ds(3 * C, K - 3 * C), :] = jnp.zeros((3, K - 3 * C, C), BF16)
            arrived(wf.at[k, :, pl.ds(0, 3 * C)], w_sem.at[k])
            tails = [wf[k, a, :, LOW:C] for a in range(3)] + [jnp.zeros((K, TAIL), BF16)]
            for i in range(2):
                wt[k, :, pl.ds(128 * i, 128)] = jnp.concatenate(
                    tails[2 * i : 2 * i + 2], axis=1
                )
        arrived(vecs, v_sem.at[0])
        arrived(emb, v_sem.at[1])
        for row, i in enumerate((0, 1, 3, 4)):
            wide[row : row + 1, :] = widen(vecs[i] * 0.5)

    for s in range(2):
        into = sums.at[slots(s, 0, 1)]
        send_sums(s, total, msg.at[s], into, ar_send, ar_recv.at[s])
        if s == 0:
            prepare()
        else:
            arrived(halo.at[0], halo_recv.at[0])
            arrived(corner.at[0], cor_recv.at[0])
            arrange(0, xv)
        total = take_sums(total, into, ar_recv.at[s])
    for h in range(2):
        coefficients(0, h, total[h : h + 1])
    arrived(sums, ar_send)
    arrived(halo.at[0], halo_send)
    arrived(corner.at[0], cor_send)

    totals = [None, None]
    activate(0)
    for f in range(F):
        acc = convolve(0, f)
        if f + 1 < F:
            activate(f + 1)
        acc = acc + (vecs[2] + emb[f : f + 1, :])
        rounded = acc.astype(BF16).reshape(T, T, C)
        hid[f] = rounded
        note_frame(f, rounded.astype(F32))
        if f % 2 == 1:
            h = f // 2
            totals[h] = local_sums()[h : h + 1]
            into = sums2.at[slots(0, h, 2)]
            send_sums(0, totals[h], msg2.at[0, h], into, ar_send2, ar_recv2.at[0, h])
    exchange(1, hid)
    for h in range(2):
        totals[h] = take_sums(totals[h], sums2.at[slots(0, h, 2)], ar_recv2.at[0, h])
        into = sums2.at[slots(1, h, 2)]
        send_sums(1, totals[h], msg2.at[1, h], into, ar_send2, ar_recv2.at[1, h])
    arrived(halo.at[1], halo_recv.at[1])
    arrived(corner.at[1], cor_recv.at[1])
    arrange(1, hid)
    arrived(halo.at[1], halo_send)
    arrived(corner.at[1], cor_send)

    for h in range(2):
        totals[h] = take_sums(totals[h], sums2.at[slots(1, h, 2)], ar_recv2.at[1, h])
        coefficients(1, h, totals[h])
        activate(2 * h)
        for f in (2 * h, 2 * h + 1):
            acc = convolve(1, f)
            if f == 2 * h:
                activate(f + 1)
            acc = acc + vecs[5] + xv[f].astype(F32).reshape(T * T, C)
            o_ref[f] = acc.astype(BF16).reshape(T, T, C)
    arrived(sums2, ar_send2)


def block(n_lon, n_lat, *args):
    vm = pltpu.VMEM
    hbm = pl.BlockSpec(memory_space=pltpu.HBM)
    dma = pltpu.SemaphoreType.DMA
    n_peers = n_lon // 2 - 1 + 2 * n_lat - 1
    return pl.pallas_call(
        functools.partial(kernel, n_lon, n_lat),
        out_shape=jax.ShapeDtypeStruct((F, T, T, C), BF16),
        in_specs=[hbm] * 10,
        out_specs=pl.BlockSpec(memory_space=vm),
        scratch_shapes=[
            vm((F, T, T, C), BF16),
            vm((F, T, T, C), BF16),
            vm((2, 3, K, C), BF16),
            vm((2, K, 256), BF16),
            vm((F, 18 * T, K), BF16),
            vm((F, 18 * T, K), BF16),
            vm((C, 128), BF16),
            vm((128, K), BF16),
            vm((4, K), F32),
            vm((8, C), F32),
            vm((8, K), F32),
            vm((6, 1, C), F32),
            vm((F, C), F32),
            vm((2, 2, 128), F32),
            vm((2, 2, 1, 128), F32),
            vm((n_peers, 2, 128), F32),
            vm((2 * n_peers, 1, 128), F32),
            vm((2, 4, F, T, C), BF16),
            vm((2, 2, 2, F, C), F32),
            vm((2, F, T, C), BF16),
            vm((2, 2, F, C), F32),
            dma,
            dma((2,)),
            dma((2,)),
            dma,
            dma((2,)),
            dma,
            dma((2, 2)),
            dma,
            dma((2,)),
            dma,
            dma((2,)),
        ],
        compiler_params=pltpu.CompilerParams(collective_id=0, has_side_effects=True, vmem_limit_bytes=24 * 2**20),
    )(*[pltpu.with_memory_space_constraint(a, pltpu.HBM) for a in args])


def solution(mesh):
    n_lon, n_lat = mesh.shape["lon"], mesh.shape["lat"]
    tile = P(None, "lat", "lon", None)
    return jax.shard_map(
        functools.partial(block, n_lon, n_lat),
        mesh=mesh,
        in_specs=(tile,) + (P(),) * 9,
        out_specs=tile,
        check_vma=False,
    )
```

```python
import functools

import jax
import jax.numpy as jnp
from jax import lax
from jax.experimental import pallas as pl
from jax.experimental.pallas import tpu as pltpu
from jax.sharding import PartitionSpec as P

GROUPS = 32
F = 4
T = 16
C = 320
LOW = 256
TAIL = C - LOW
K = 1024
F32 = jnp.float32
BF16 = jnp.bfloat16
MESH = pl.DeviceIdType.MESH


def kernel(
    n_lon,
    n_lat,
    x_hbm,
    g1_hbm,
    s1_hbm,
    w1_hbm,
    b1_hbm,
    emb_hbm,
    g2_hbm,
    s2_hbm,
    w2_hbm,
    b2_hbm,
    o_ref,
    xv,
    hid,
    wf,
    wt,
    raw,
    cols,
    to_groups,
    to_lanes,
    wide,
    stat,
    coef,
    vecs,
    emb,
    msg,
    msg2,
    sums,
    sums2,
    halo,
    corner,
    colsend,
    corsend,
    x_sem,
    w_sem,
    v_sem,
    ar_send,
    ar_recv,
    ar_send2,
    ar_recv2,
    halo_send,
    halo_recv,
    cor_send,
    cor_recv,
):
    n_y, n_z, half = n_lon // 4, n_lat // 2, n_lon // 2
    rem, div = lax.rem, lax.div
    lon, lat = lax.axis_index("lon"), lax.axis_index("lat")
    y, x_hi, core = div(lon, 4), rem(div(lon, 2), 2), rem(lon, 2)
    x_lo, z = div(lat, n_z), rem(lat, n_z)

    def flip(bit, on):
        return 1 - bit if on else bit

    def hops(step, n):
        return min(step, n - step)

    x_hops = (0, 2, 1, 1)
    stages = [[], []]
    for d in sorted(range(1, 2 * n_y), key=lambda d: -hops(d // 2, n_y)):
        to_y = rem(y + d // 2, n_y)
        stages[0].append((to_y * 4 + x_hi * 2 + flip(core, d % 2), lat))
    for d in sorted(range(1, 4 * n_z), key=lambda d: -hops(d // 4, n_z) - x_hops[d % 4]):
        to_z = rem(z + d // 4, n_z)
        to_lon = y * 4 + flip(x_hi, d & 1) * 2 + core
        stages[1].append((to_lon, flip(x_lo, d & 2) * n_z + to_z))

    at_pole = [(lat == 0).astype(jnp.int32), (lat == n_lat - 1).astype(jnp.int32)]
    row_lat = [lat - 1 + at_pole[0], lat + 1 - at_pole[1]]
    row_shift = [half * at_pole[0], half * at_pole[1]]
    row_side = [1 - at_pole[0], at_pole[1]]
    row_dev = [(rem(lon + row_shift[v], n_lon), row_lat[v]) for v in range(2)]
    col_dev = [(rem(lon + n_lon - 1, n_lon), lat), (rem(lon + 1, n_lon), lat)]
    cor_dev = [
        [(rem(lon + row_shift[v] + n_lon + (2 * h - 1), n_lon), row_lat[v]) for h in range(2)]
        for v in range(2)
    ]

    greeted = stages[1] + stages[0] + cor_dev[0] + cor_dev[1] + row_dev + col_dev
    barrier = pltpu.get_barrier_semaphore()
    for dev in greeted:
        pl.semaphore_signal(barrier, inc=1, device_id=dev, device_id_type=MESH)
    for f in range(F):
        pltpu.make_async_copy(x_hbm.at[f], xv.at[f], x_sem).start()

    vec_in = [
        pltpu.make_async_copy(hbm, vecs.at[i, 0], v_sem.at[0])
        for i, hbm in enumerate((g1_hbm, s1_hbm, b1_hbm, g2_hbm, s2_hbm, b2_hbm))
    ]
    vec_in.append(pltpu.make_async_copy(emb_hbm, emb, v_sem.at[1]))
    for cp in vec_in:
        cp.start()
    for k, hbm in enumerate((w1_hbm, w2_hbm)):
        for a in range(3):
            for b in range(3):
                pltpu.make_async_copy(
                    hbm.at[a, b, pl.ds(0, LOW)], wf.at[k, a, pl.ds(b * LOW, LOW)], w_sem.at[k]
                ).start()
                pltpu.make_async_copy(
                    hbm.at[a, b, pl.ds(LOW, TAIL)],
                    wf.at[k, a, pl.ds(3 * LOW + b * TAIL, TAIL)],
                    w_sem.at[k],
                ).start()

    per = C // GROUPS

    def member(chan, group):
        inside = (chan >= group * per) & (chan < group * per + per)
        return jnp.where(inside, 1.0, 0.0).astype(BF16)

    def iota(shape, dim):
        return lax.broadcasted_iota(jnp.int32, shape, dim)

    own_lanes = (lax.broadcasted_iota(jnp.int32, (8, 128), 0) & 3) == (
        lax.broadcasted_iota(jnp.int32, (8, 128), 1) // GROUPS
    )
    own_low_lanes = (lax.broadcasted_iota(jnp.int32, (8, 128), 0) & 1) == (
        lax.broadcasted_iota(jnp.int32, (8, 128), 1) // GROUPS
    )

    def select(v, chosen):
        high = v.astype(BF16).astype(F32)
        middle = (v - high).astype(BF16).astype(F32)
        low = v - high - middle
        parts = jnp.concatenate([high, middle, low], axis=0).astype(BF16)
        out = jnp.dot(parts, chosen, preferred_element_type=F32)
        return out[0:8] + out[8:16] + out[16:24]

    def note_frame(f, v):
        flat = v.reshape(T * T, C)
        row = div(f, 2) * 4 + rem(f, 2)
        stat[pl.ds(row, 1), :] = jnp.sum(flat, axis=0, keepdims=True)
        stat[pl.ds(row + 2, 1), :] = jnp.sum(flat * flat, axis=0, keepdims=True)

    def note_edges(f, v):
        for h, c in enumerate((0, T - 1)):
            column = v[:, c, :]
            colsend[h, f] = column.astype(BF16)
            for side, r in enumerate((0, T - 1)):
                corsend[side, h, pl.ds(f, 1), :] = column[r : r + 1, :]

    def remote(src, dst, send, recv, dev):
        pltpu.make_async_remote_copy(
            src_ref=src,
            dst_ref=dst,
            send_sem=send,
            recv_sem=recv,
            device_id=dev,
            device_id_type=MESH,
        ).start()

    def arrived(ref, sem):
        pltpu.make_async_copy(ref, ref, sem).wait()

    def exchange(p, src):
        for v, r in enumerate((0, T - 1)):
            remote(
                src.at[:, r], halo.at[p, row_side[v]], halo_send, halo_recv.at[p], row_dev[v]
            )

        def edges(f, carry):
            note_edges(f, src[f].astype(F32))
            return carry

        lax.fori_loop(0, F, edges, 0)
        for v in range(2):
            for h in range(2):
                remote(
                    corsend.at[v, h],
                    corner.at[p, row_side[v], 1 - h],
                    cor_send,
                    cor_recv.at[p],
                    cor_dev[v][h],
                )
        for h in range(2):
            remote(colsend.at[h], halo.at[p, 3 - h], halo_send, halo_recv.at[p], col_dev[h])

    def local_sums():
        picked = jnp.where(own_lanes, select(stat[...], to_groups[...]), 0.0)
        return jnp.concatenate(
            [jnp.sum(picked[4 * h : 4 * h + 4], axis=0, keepdims=True) for h in range(2)], axis=0
        )

    def slots(s, h, n_halves):
        n = [len(stage) for stage in stages]
        return pl.ds(n[0] * h if s == 0 else n[0] * n_halves + n[1] * h, n[s])

    def send_sums(s, total, out, into, send, recv):
        out[...] = total
        for i, dev in enumerate(stages[s]):
            remote(out, into.at[i], send, recv, dev)

    def take_sums(total, into, recv):
        arrived(into, recv)
        return total + jnp.sum(into[...], axis=0)

    def coefficients(p, h, total):
        count = float(T * T * n_lon * n_lat * per)
        average = total / count
        variance = pltpu.roll(average, 64, 1) - average * average
        inverse = lax.rsqrt(jnp.maximum(variance, 0.0) + 1e-05)
        both = jnp.concatenate(
            [jnp.broadcast_to(average, (2, 128)), jnp.broadcast_to(inverse, (2, 128))] * 2, axis=0
        )
        spread = select(jnp.where(own_low_lanes, both, 0.0), to_lanes[...])
        scale = spread[2:4] * wide[2 * p : 2 * p + 1, :]
        coef[4 * h : 4 * h + 2, :] = wide[2 * p + 1 : 2 * p + 2, :] - spread[0:2] * scale
        coef[4 * h + 2 : 4 * h + 4, :] = scale

    def widen(v):
        return jnp.concatenate(
            [v[:, :LOW]] * 3 + [v[:, LOW:]] * 3 + [jnp.zeros((1, K - 3 * C), F32)], axis=1
        )

    def arrange(p, src):
        def one(f, carry):
            rows = jnp.concatenate([halo[p, 0, f][None], src[f], halo[p, 1, f][None]], axis=0)
            mid = rows.astype(F32)
            side = []
            for h in range(2):
                strip = jnp.concatenate(
                    [
                        corner[p, 0, h, pl.ds(f, 1), :],
                        halo[p, 2 + h, f].astype(F32),
                        corner[p, 1, h, pl.ds(f, 1), :],
                    ],
                    axis=0,
                )
                side.append(strip[:, None, :])
            west = jnp.concatenate([side[0], mid[:, : T - 1, :]], axis=1)
            east = jnp.concatenate([mid[:, 1:, :], side[1]], axis=1)
            taps = [v.reshape(18 * T, C) for v in (west, mid, east)]
            for b, v in enumerate(taps):
                raw[f, :, pl.ds(b * LOW, LOW)] = v[:, :LOW].astype(BF16)
            tails = [v[:, LOW:] for v in taps] + [jnp.zeros((18 * T, TAIL), F32)]
            for i in range(2):
                pair = jnp.concatenate(tails[2 * i : 2 * i + 2], axis=1)
                raw[f, :, pl.ds(3 * LOW + 128 * i, 128)] = pair.astype(BF16)
            return carry

        lax.fori_loop(0, F, one, 0)

    def activate(f):
        row = f // 2 * 4 + f % 2
        for i in range(K // LOW):
            lanes = pl.ds(i * LOW, LOW)
            v = raw[f, :, lanes].astype(F32)
            h = v * coef[row + 2 : row + 3, lanes] + coef[row : row + 1, lanes]
            cols[f, :, lanes] = (h + h * jnp.tanh(h)).astype(BF16)

    def convolve(k, f):
        low = jnp.zeros((T * T, LOW), F32)
        for a in range(3):
            low += jnp.dot(
                cols[f, pl.ds(a * T, T * T), :], wf[k, a, :, 0:LOW], preferred_element_type=F32
            )
        side = jnp.dot(cols[f], wt[k], preferred_element_type=F32)
        tail = side[0 : T * T, 0:TAIL]
        tail = tail + side[T : T + T * T, TAIL : 2 * TAIL]
        tail = tail + side[2 * T : 2 * T + T * T, 2 * TAIL : 3 * TAIL]
        return jnp.concatenate([low, tail], axis=1)

    arrived(xv, x_sem)

    def first_notes(f, carry):
        note_frame(f, xv[f].astype(F32))
        return carry

    lax.fori_loop(0, F, first_notes, 0)
    to_groups[...] = member(iota((C, 128), 0), iota((C, 128), 1) & (GROUPS - 1))
    total = local_sums()
    pl.semaphore_wait(barrier, len(greeted))

    def prepare():
        exchange(0, xv)
        lane = iota((128, K), 1)
        chan = jnp.where(lane < 3 * LOW, lane & (LOW - 1), LOW + (lane & (TAIL - 1)))
        chan = jnp.where(lane < 3 * C, chan, -1)
        to_lanes[...] = member(chan, iota((128, K), 0) & (GROUPS - 1))
        for k in range(2):
            wf[k, :, pl.ds(3 * C, K - 3 * C), :] = jnp.zeros((3, K - 3 * C, C), BF16)
            arrived(wf.at[k, :, pl.ds(0, 3 * C)], w_sem.at[k])
            tails = [wf[k, a, :, LOW:C] for a in range(3)] + [jnp.zeros((K, TAIL), BF16)]
            for i in range(2):
                wt[k, :, pl.ds(128 * i, 128)] = jnp.concatenate(
                    tails[2 * i : 2 * i + 2], axis=1
                )
        arrived(vecs, v_sem.at[0])
        arrived(emb, v_sem.at[1])
        for row, i in enumerate((0, 1, 3, 4)):
            wide[row : row + 1, :] = widen(vecs[i] * 0.5)

    for s in range(2):
        into = sums.at[slots(s, 0, 1)]
        send_sums(s, total, msg.at[s], into, ar_send, ar_recv.at[s])
        if s == 0:
            prepare()
        else:
            arrived(halo.at[0], halo_recv.at[0])
            arrived(corner.at[0], cor_recv.at[0])
            arrange(0, xv)
        total = take_sums(total, into, ar_recv.at[s])
    for h in range(2):
        coefficients(0, h, total[h : h + 1])
    arrived(sums, ar_send)
    arrived(halo.at[0], halo_send)
    arrived(corner.at[0], cor_send)

    totals = [None, None]
    for f in range(F):
        if f % 2 == 0:
            activate(f)
        acc = convolve(0, f)
        if f % 2 == 0:
            activate(f + 1)
        acc = acc + (vecs[2] + emb[f : f + 1, :])
        rounded = acc.astype(BF16).reshape(T, T, C)
        hid[f] = rounded
        note_frame(f, rounded.astype(F32))
        if f % 2 == 1:
            h = f // 2
            totals[h] = local_sums()[h : h + 1]
            into = sums2.at[slots(0, h, 2)]
            send_sums(0, totals[h], msg2.at[0, h], into, ar_send2, ar_recv2.at[0, h])
    exchange(1, hid)
    for h in range(2):
        totals[h] = take_sums(totals[h], sums2.at[slots(0, h, 2)], ar_recv2.at[0, h])
        into = sums2.at[slots(1, h, 2)]
        send_sums(1, totals[h], msg2.at[1, h], into, ar_send2, ar_recv2.at[1, h])
    arrived(halo.at[1], halo_recv.at[1])
    arrived(corner.at[1], cor_recv.at[1])
    arrange(1, hid)
    arrived(halo.at[1], halo_send)
    arrived(corner.at[1], cor_send)

    for h in range(2):
        totals[h] = take_sums(totals[h], sums2.at[slots(1, h, 2)], ar_recv2.at[1, h])
        coefficients(1, h, totals[h])
        activate(2 * h)
        for f in (2 * h, 2 * h + 1):
            acc = convolve(1, f)
            if f == 2 * h:
                activate(f + 1)
            acc = acc + vecs[5] + xv[f].astype(F32).reshape(T * T, C)
            o_ref[f] = acc.astype(BF16).reshape(T, T, C)
    arrived(sums2, ar_send2)


def block(n_lon, n_lat, *args):
    vm = pltpu.VMEM
    hbm = pl.BlockSpec(memory_space=pltpu.HBM)
    dma = pltpu.SemaphoreType.DMA
    n_peers = n_lon // 2 - 1 + 2 * n_lat - 1
    return pl.pallas_call(
        functools.partial(kernel, n_lon, n_lat),
        out_shape=jax.ShapeDtypeStruct((F, T, T, C), BF16),
        in_specs=[hbm] * 10,
        out_specs=pl.BlockSpec(memory_space=vm),
        scratch_shapes=[
            vm((F, T, T, C), BF16),
            vm((F, T, T, C), BF16),
            vm((2, 3, K, C), BF16),
            vm((2, K, 256), BF16),
            vm((F, 18 * T, K), BF16),
            vm((F, 18 * T, K), BF16),
            vm((C, 128), BF16),
            vm((128, K), BF16),
            vm((4, K), F32),
            vm((8, C), F32),
            vm((8, K), F32),
            vm((6, 1, C), F32),
            vm((F, C), F32),
            vm((2, 2, 128), F32),
            vm((2, 2, 1, 128), F32),
            vm((n_peers, 2, 128), F32),
            vm((2 * n_peers, 1, 128), F32),
            vm((2, 4, F, T, C), BF16),
            vm((2, 2, 2, F, C), F32),
            vm((2, F, T, C), BF16),
            vm((2, 2, F, C), F32),
            dma,
            dma((2,)),
            dma((2,)),
            dma,
            dma((2,)),
            dma,
            dma((2, 2)),
            dma,
            dma((2,)),
            dma,
            dma((2,)),
        ],
        compiler_params=pltpu.CompilerParams(collective_id=0, has_side_effects=True, vmem_limit_bytes=24 * 2**20),
    )(*[pltpu.with_memory_space_constraint(a, pltpu.HBM) for a in args])


def solution(mesh):
    n_lon, n_lat = mesh.shape["lon"], mesh.shape["lat"]
    tile = P(None, "lat", "lon", None)
    return jax.shard_map(
        functools.partial(block, n_lon, n_lat),
        mesh=mesh,
        in_specs=(tile,) + (P(),) * 9,
        out_specs=tile,
        check_vma=False,
    )
```
